256 devices in a mesh: cosmo: 2 (over z), row: 128 (over y, x, core).
Axes of the slice: x: 8, y: 8, z: 2, core: 2. Of those that a mesh axis runs over, the one named last changes fastest.
The devices are a block of a 8x8x16 slice.
Arguments:
- potentials: float32 [4, 2048, 16384], P('cosmo', 'row'), parts along dimension 0, may hold values from -3 to 3
- ratios: float32 [6], P('cosmo'), parts along dimension 0, may hold values from 0.3 to 0.9
- row_offset: int32 [256], P('cosmo'), parts along dimension 0, may hold values from 0 to 7
- col_offset: int32 [256], P('cosmo'), parts along dimension 0, may hold values from 0 to 127
Outputs:
- convergence: float32 [4096, 16384], P(('cosmo', 'row')), parts along dimension 0
- shear_map: float32 [2, 4096, 16384], P(None, ('cosmo', 'row')), parts along dimension 1
- rotation: float32 [4096, 16384], P(('cosmo', 'row')), parts along dimension 0
- displacement: float32 [2, 4096, 16384], P(None, ('cosmo', 'row')), parts along dimension 1
The draws below stay inside these ranges and needn't reach their ends.
There are 2 independent parts, one for each index of `cosmo`. The reference program is written for one: setup_inputs(seed, part) draws one part's arguments, and reference() takes and returns one part's arrays. A program takes and returns all parts, laid end to end along the dimension named above; each array names one. Nothing has to cross between parts.
Inputs may be any that keep to these rules, and one draw needn't show every extreme that they name: `row_offset`: row offsets count blocks of 256 rows.
All inputs are finite; a program needn't handle non-finite values.
Results may differ from the reference program's by a relative error of at most 0.00002.
Values sent between devices are 32-bit elements; how exact they have to be, the bound alone decides.
No kernel may reach another device: no remote copies, remote signals or barrier semaphores. Data moves between devices by JAX's collectives and lax.ppermute only.
A program may use at most 128 MiB of HBM per device.

```python
import jax
import jax.numpy as jnp

NC = 16384
PLANES = 2
RB = 8
NR = 2048
NCB = 128


def plant(entries, own_key, smallest, high):
    spot = [jax.random.randint(jax.random.fold_in(own_key, axis), (), 0, length) for axis, length in enumerate(entries.shape)]
    main_axis = entries.shape.index(max(entries.shape))
    neighbour = spot[:main_axis] + [(spot[main_axis] + 1) % entries.shape[main_axis]] + spot[main_axis + 1:]
    return entries.at[tuple(spot)].set(smallest).at[tuple(neighbour)].set(high)


def level_of(key, dims, split, smallest, largest):
    level = 1.0
    for position, shards_of in split:
        draws = jax.random.uniform(jax.random.fold_in(jax.random.fold_in(key, 6), position), (shards_of,), jnp.float32, smallest / len(split), largest / len(split))
        level = level * jnp.repeat(jnp.exp(draws), dims[position] // shards_of).reshape((-1,) + (1,) * (len(dims) - 1 - position))
    return level


def centred(own_key, shape, spread, reach, cuts=(), kind=jnp.bfloat16):
    values = jax.random.normal(own_key, shape, jnp.float32) * spread
    if len(cuts) > 0:
        values = level_of(own_key, shape, cuts, -0.22, 0.18) * values
    return jnp.clip(values, min=-reach, max=reach).astype(kind)


def setup_inputs(seed: int = 0, part: int = 0) -> dict:
    splits = jax.random.split(jax.random.key(seed), 5)
    part_keys = jax.random.split(jax.random.fold_in(splits[4], part), 5)
    potentials = centred(part_keys[0], (PLANES, NR, NC), 0.5, 3.0, ((1, 128),), jnp.float32)
    ratios = jnp.clip(jax.random.uniform(part_keys[1], (3,), jnp.float32, 0.3, 0.9), 0.3, 0.9)
    row_offset = plant(jax.random.randint(part_keys[2], (NCB,), 0, RB), jax.random.fold_in(part_keys[2], 1), 0, RB - 1).astype(jnp.int32)
    col_offset = plant(jax.random.randint(part_keys[3], (NCB,), 0, NCB), jax.random.fold_in(part_keys[3], 1), 0, NCB - 1).astype(jnp.int32)
    return {"potentials": potentials, "ratios": ratios, "row_offset": row_offset, "col_offset": col_offset}


def slope_along(field, direction):
    return (8.0 * (jnp.roll(field, -1, direction) - jnp.roll(field, 1, direction)) - (jnp.roll(field, -2, direction) - jnp.roll(field, 2, direction))) / 12.0


def derive_plane(potential):
    slope_r = slope_along(potential, 0)
    slope_c = slope_along(potential, 1)
    return (slope_r, slope_c, slope_along(slope_r, 0), slope_along(slope_r, 1), slope_along(slope_c, 1))


def assemble(nearer, farther, ratios):
    near_r, near_c, near_rr, near_rc, near_cc = nearer
    far_r, far_c, far_rr, far_rc, far_cc = farther
    beta_near = ratios[0]
    beta_one = ratios[1]
    beta_two = ratios[2]
    inner_rr = 1.0 - beta_near * near_rr
    inner_rc = -beta_near * near_rc
    inner_cc = 1.0 - beta_near * near_cc
    chain_rr = far_rr * inner_rr + far_rc * inner_rc
    chain_rc = far_rr * inner_rc + far_rc * inner_cc
    chain_cr = far_rc * inner_rr + far_cc * inner_rc
    chain_cc = far_rc * inner_rc + far_cc * inner_cc
    total_rr = 1.0 - beta_one * near_rr - beta_two * chain_rr
    total_rc = -beta_one * near_rc - beta_two * chain_rc
    total_cr = -beta_one * near_rc - beta_two * chain_cr
    total_cc = 1.0 - beta_one * near_cc - beta_two * chain_cc
    convergence = 1.0 - 0.5 * (total_rr + total_cc)
    shear_map = jnp.stack([0.5 * (total_rr - total_cc), -0.5 * (total_rc + total_cr)])
    rotation = 0.5 * (total_rc - total_cr)
    displacement = jnp.stack([beta_one * near_r + beta_two * far_r, beta_one * near_c + beta_two * far_c])
    return convergence, shear_map, rotation, displacement


def reference(potentials, ratios, row_offset, col_offset):
    nearer = derive_plane(potentials[0])
    derived = derive_plane(potentials[1])
    blocks = NC // 128
    source = (jnp.arange(blocks, dtype=jnp.int32) + col_offset.astype(jnp.int32)) % blocks
    lookup_rows = (jnp.arange(NR, dtype=jnp.int32)[:, None] + (NR // RB) * row_offset.astype(jnp.int32)[None, :]) % NR

    def sample(field):
        strips = field.reshape(NR, blocks, 128)
        return strips[lookup_rows, source[None, :], :].reshape(NR, NC)

    farther = tuple(sample(member) for member in derived)
    return assemble(nearer, farther, ratios)
```

```python
import functools

import jax
import jax.numpy as jnp
from jax import lax
from jax.experimental import pallas as pl
from jax.experimental.pallas import tpu as pltpu
from jax.sharding import PartitionSpec as P

RB = 8
LANES = 128
EDGE = 8
STRIDE = 32
CAPS = (16, 18, 20, 22, 24, 28, 32, 48, 128)
C1, C2 = 8.0 / 12.0, 1.0 / 12.0
VMEM = pl.BlockSpec(memory_space=pltpu.VMEM)
SMEM = pl.BlockSpec(memory_space=pltpu.SMEM)


def lanes_of(rows):
    return lax.broadcasted_iota(jnp.int32, (rows, LANES), 1)


def params(mib):
    return pltpu.CompilerParams(vmem_limit_bytes=mib * 2**20)


def tiles_of(cap):
    return 2 * cap + -(-cap // 8)


def first(ahead, behind, ahead2, behind2):
    return C1 * (ahead - behind) - C2 * (ahead2 - behind2)


def second(centre, pairs):
    one, two, three, four = pairs
    return (four - 16.0 * three + 64.0 * two + 16.0 * one - 130.0 * centre) * (1.0 / 144.0)


def rows_of(window):
    def at(k):
        return window[8 + k : 24 + k, :]

    a1, b1, a2, b2 = at(1), at(-1), at(2), at(-2)
    slope = first(a1, b1, a2, b2)
    curve = second(at(0), (a1 + b1, a2 + b2, at(3) + at(-3), at(4) + at(-4)))
    return slope, curve


def slope_rows(window):
    def at(k):
        return window[8 + k : 24 + k, :]

    return first(at(1), at(-1), at(2), at(-2))


def shifted(field, beside, k, lane):
    if k > 0:
        return pltpu.roll(jnp.where(lane < k, beside, field), LANES - k, 1)
    return pltpu.roll(jnp.where(lane >= LANES + k, beside, field), -k, 1)


def columns_of(field, beside, slope, slope_beside, lane):
    def at(k):
        return shifted(field, beside, k, lane)

    a1, b1, a2, b2 = at(1), at(-1), at(2), at(-2)
    slope_c = first(a1, b1, a2, b2)
    curve_cc = second(field, (a1 + b1, a2 + b2, at(3) + at(-3), at(4) + at(-4)))

    def of_slope(k):
        return shifted(slope, slope_beside, k, lane)

    curve_rc = first(of_slope(1), of_slope(-1), of_slope(2), of_slope(-2))
    return slope_c, curve_rc, curve_cc


def near_kernel(blocks, p_ref, up_ref, down_ref, r_ref, c_ref, rr_ref, rc_ref, cc_ref, f_ref):
    lane = lanes_of(16)

    def rows(b, _):
        col = pl.multiple_of(b * LANES, LANES)
        base = pl.multiple_of(b * STRIDE, STRIDE)
        out = pl.multiple_of(b * 16, 16)
        window = f_ref.at[pl.ds(base, STRIDE), :]
        window[4:8, :] = up_ref[:, pl.ds(col, LANES)]
        window[8:24, :] = p_ref[:, pl.ds(col, LANES)]
        window[24:28, :] = down_ref[:, pl.ds(col, LANES)]
        slope, curve = rows_of(window)
        r_ref[pl.ds(out, 16), :] = slope
        rr_ref[pl.ds(out, 16), :] = curve
        return 0

    lax.fori_loop(0, blocks, rows, 0, unroll=4)

    def columns(b, _):
        before = lax.rem(b + (blocks - 1), blocks)
        after = lax.rem(b + 1, blocks)

        def of(i):
            return p_ref[:, pl.ds(pl.multiple_of(i * LANES, LANES), LANES)]

        def slope_of(i):
            return r_ref[pl.ds(pl.multiple_of(i * 16, 16), 16), :]

        far = lane >= LANES // 2
        slope_c, curve_rc, curve_cc = columns_of(
            of(b),
            jnp.where(far, of(before), of(after)),
            slope_of(b),
            jnp.where(far, slope_of(before), slope_of(after)),
            lane,
        )
        out = pl.ds(pl.multiple_of(b * 16, 16), 16)
        c_ref[out, :] = slope_c
        rc_ref[out, :] = curve_rc
        cc_ref[out, :] = curve_cc
        return 0

    lax.fori_loop(0, blocks, columns, 0, unroll=2)


def near_fields(potentials, up, down):
    height, width = potentials.shape[1:]
    blocks = width // LANES
    shape = jax.ShapeDtypeStruct((blocks * 16, LANES), jnp.float32)
    return pl.pallas_call(
        functools.partial(near_kernel, blocks),
        grid=(1,),
        out_shape=(shape,) * 5,
        in_specs=[pl.BlockSpec((None, height, width), lambda i: (0, 0, 0)), VMEM, VMEM],
        out_specs=(VMEM,) * 5,
        scratch_shapes=[pltpu.VMEM((blocks * STRIDE, LANES), jnp.float32)],
        compiler_params=params(16),
        cost_estimate=pl.CostEstimate(flops=60_000_000, bytes_accessed=7_000_000, transcendentals=0),
        name="near_fields",
    )(potentials, up, down)


def pack_kernel(blocks, cap, where_ref, shift_ref, slot_ref, source_ref, p_ref, out_ref):
    here = where_ref[0]
    tall = tiles_of(cap) * 8
    lane = lanes_of(8)
    far = lane >= LANES // 2

    def block(b, _):
        slot = slot_ref[b]
        source = source_ref[b]
        start = lax.rem(here + RB - shift_ref[b], RB) * tall
        before = lax.rem(source + (blocks - 1), blocks)
        after = lax.rem(source + 1, blocks)

        def of(i):
            return p_ref[:, pl.ds(pl.multiple_of(i * LANES, LANES), LANES)]

        out_ref[pl.ds(pl.multiple_of(start + slot * 16, 8), 16), :] = of(source)
        left, right = of(before), of(after)
        place = lax.rem(slot, 8) * EDGE
        row = pl.ds(pl.multiple_of(start + 16 * cap + lax.div(slot, 8) * 8, 8), 8)
        for half in range(2):
            top = 8 * half
            edge = jnp.where(far, left[top : top + 8], right[top : top + 8])
            spot = place + half * (LANES // 2)
            moved = pltpu.roll(edge, spot + EDGE // 2, 1)
            mask = (lane >= spot) & (lane < spot + EDGE)
            pltpu.store(out_ref.at[row, :], moved, mask=mask)
        return 0

    lax.fori_loop(0, blocks, block, 0, unroll=4)


def pack(cap, where, shift, slot, source, potentials):
    height, width = potentials.shape[1:]
    blocks = width // LANES
    return pl.pallas_call(
        functools.partial(pack_kernel, blocks, cap),
        grid=(1,),
        out_shape=jax.ShapeDtypeStruct((RB * tiles_of(cap) * 8, LANES), jnp.float32),
        in_specs=[SMEM] * 4 + [pl.BlockSpec((None, height, width), lambda i: (1, 0, 0))],
        out_specs=VMEM,
        compiler_params=params(16),
        cost_estimate=pl.CostEstimate(flops=2_000_000, bytes_accessed=3_000_000, transcendentals=0),
        name="pack_blocks",
    )(where, shift, slot, source, potentials)


def unpack_kernel(blocks, cap, where_ref, shift_ref, slot_ref, in_ref, w_ref, h_ref, head_ref, tail_ref):
    here = where_ref[0]
    tall = tiles_of(cap) * 8
    lane = lanes_of(8)

    def block(b, _):
        slot = slot_ref[b]
        start = lax.rem(here + shift_ref[b], RB) * tall
        tile = in_ref[pl.ds(pl.multiple_of(start + slot * 16, 8), 16), :]
        col = pl.ds(pl.multiple_of(b * LANES, LANES), LANES)
        w_ref[pl.ds(pl.multiple_of(b * 16, 16), 16), :] = tile
        head_ref[:, col] = tile[0:4]
        tail_ref[:, col] = tile[12:16]
        edge = in_ref[pl.ds(pl.multiple_of(start + 16 * cap + lax.div(slot, 8) * 8, 8), 8), :]
        place = lax.rem(slot, 8) * EDGE
        spot = lax.rem(b, 16) * EDGE
        mask = (lane >= spot) & (lane < spot + EDGE)
        for half in range(2):
            turn = lax.rem(spot + 2 * LANES - place - half * (LANES // 2), LANES)
            row = pl.ds(pl.multiple_of(lax.div(b, 16) * 16 + 8 * half, 8), 8)
            pltpu.store(h_ref.at[row, :], pltpu.roll(edge, turn, 1), mask=mask)
        return 0

    lax.fori_loop(0, blocks, block, 0, unroll=4)
    for g in range(blocks // 16):
        col = slice((blocks + g) * LANES, (blocks + g + 1) * LANES)
        head_ref[:, col] = h_ref[16 * g : 16 * g + 4, :]
        tail_ref[:, col] = h_ref[16 * g + 12 : 16 * g + 16, :]


def unpack(cap, blocks, where, shift, slot, arrived):
    ends = jax.ShapeDtypeStruct((4, (blocks + blocks // 16) * LANES), jnp.float32)
    return pl.pallas_call(
        functools.partial(unpack_kernel, blocks, cap),
        out_shape=(
            jax.ShapeDtypeStruct((blocks * 16, LANES), jnp.float32),
            jax.ShapeDtypeStruct((blocks, LANES), jnp.float32),
            ends,
            ends,
        ),
        in_specs=[SMEM] * 3 + [VMEM],
        out_specs=(VMEM,) * 4,
        compiler_params=params(16),
        cost_estimate=pl.CostEstimate(flops=2_000_000, bytes_accessed=3_000_000, transcendentals=0),
        name="unpack_blocks",
    )(where, shift, slot, arrived)


def far_kernel(
    ratio_ref, w_ref, h_ref, up_ref, down_ref, uph_ref, downh_ref, r_ref, c_ref, rr_ref, rc_ref, cc_ref,
    conv_ref, shear_ref, rot_ref, disp_ref, f_ref, e_ref, s_ref,
):
    lane = lanes_of(16)
    near_to_two, near_to_source, two_to_source = ratio_ref[0], ratio_ref[1], ratio_ref[2]
    half_one, half_two = 0.5 * near_to_source, 0.5 * two_to_source
    e_ref[4:8, :] = uph_ref[...]
    e_ref[8:24, :] = h_ref[...]
    e_ref[24:28, :] = downh_ref[...]
    s_ref[...] = slope_rows(e_ref)

    def block(b, _):
        col = pl.ds(pl.multiple_of(b * LANES, LANES), LANES)
        tile = pl.ds(pl.multiple_of(b * 16, 16), 16)
        window = f_ref.at[pl.ds(pl.multiple_of(b * STRIDE, STRIDE), STRIDE), :]
        centre = w_ref[tile, :]
        window[4:8, :] = up_ref[:, col]
        window[8:24, :] = centre
        window[24:28, :] = down_ref[:, col]
        far_r, far_rr = rows_of(window)
        turn = LANES - EDGE // 2 - b * EDGE
        beside = pltpu.roll(e_ref[8:24, :], turn, 1)
        slope_beside = pltpu.roll(s_ref[...], turn, 1)
        far_c, far_rc, far_cc = columns_of(centre, beside, far_r, slope_beside, lane)
        near_rr, near_rc, near_cc = rr_ref[tile, :], rc_ref[tile, :], cc_ref[tile, :]
        inner_rr = 1.0 - near_to_two * near_rr
        inner_rc = -near_to_two * near_rc
        inner_cc = 1.0 - near_to_two * near_cc
        chain_rr = far_rr * inner_rr + far_rc * inner_rc
        chain_rc = far_rr * inner_rc + far_rc * inner_cc
        chain_cr = far_rc * inner_rr + far_cc * inner_rc
        chain_cc = far_rc * inner_rc + far_cc * inner_cc
        conv_ref[:, col] = half_one * (near_rr + near_cc) + half_two * (chain_rr + chain_cc)
        shear_ref[0, :, col] = half_one * (near_cc - near_rr) + half_two * (chain_cc - chain_rr)
        shear_ref[1, :, col] = near_to_source * near_rc + half_two * (chain_rc + chain_cr)
        rot_ref[:, col] = half_two * (chain_cr - chain_rc)
        disp_ref[0, :, col] = near_to_source * r_ref[tile, :] + two_to_source * far_r
        disp_ref[1, :, col] = near_to_source * c_ref[tile, :] + two_to_source * far_c
        return 0

    lax.fori_loop(0, 16, block, 0, unroll=2)


def assemble(ratios, windows, edges, above, below, near):
    blocks = windows.shape[0] // 16
    steps = blocks // 16
    wide = 16 * LANES
    field = pl.BlockSpec((256, LANES), lambda i: (i, 0))
    ends = pl.BlockSpec((4, wide), lambda i: (0, i))
    edge_ends = pl.BlockSpec((4, LANES), lambda i: (0, blocks + i))
    flat = jax.ShapeDtypeStruct((16, blocks * LANES), jnp.float32)
    pair = jax.ShapeDtypeStruct((2, 16, blocks * LANES), jnp.float32)
    flat_spec = pl.BlockSpec((16, wide), lambda i: (0, i))
    pair_spec = pl.BlockSpec((2, 16, wide), lambda i: (0, 0, i))
    return pl.pallas_call(
        far_kernel,
        grid=(steps,),
        out_shape=(flat, pair, flat, pair),
        in_specs=[SMEM, field, pl.BlockSpec((16, LANES), lambda i: (i, 0)), ends, ends, edge_ends, edge_ends]
        + [field] * 5,
        out_specs=(flat_spec, pair_spec, flat_spec, pair_spec),
        scratch_shapes=[
            pltpu.VMEM((16 * STRIDE, LANES), jnp.float32),
            pltpu.VMEM((STRIDE, LANES), jnp.float32),
            pltpu.VMEM((16, LANES), jnp.float32),
        ],
        compiler_params=params(16),
        name="far_fields",
    )(ratios, windows, edges, above, below, above, below, *near)


def passed(x, by):
    size = lax.axis_size("row")
    return lax.ppermute(x, "row", [(i, (i + by) % size) for i in range(size)])


def per_device(potentials, ratios, row_offset, col_offset):
    devices = lax.axis_size("row")
    stride = devices // RB
    height, width = potentials.shape[1:]
    blocks = width // LANES
    index = jnp.arange(blocks, dtype=jnp.int32)
    source = (index + col_offset) % blocks
    alike = (row_offset[:, None] == row_offset[None, :]) & (index[None, :] < index[:, None])
    slot = jnp.sum(alike.astype(jnp.int32), axis=1)
    needed = jnp.max(slot) + 1
    where = (lax.axis_index("row") // stride).astype(jnp.int32).reshape(1)
    groups = [[level * stride + j for level in range(RB)] for j in range(stride)]
    above1 = passed(potentials[0, height - 4 :, :], 1)
    below1 = passed(potentials[0, :4, :], -1)
    caps = tuple(c for c in CAPS if c < blocks) + (blocks,)

    def exchange(cap, potentials, above1, below1, where, shift, slot, source):
        packed = pack(cap, where, shift, slot, source, potentials)
        packed = packed.reshape(RB, tiles_of(cap) * 8, LANES)
        arrived = lax.all_to_all(packed, "row", 0, 0, axis_index_groups=groups)
        near = near_fields(potentials, above1, below1)
        arrived = arrived.reshape(RB * tiles_of(cap) * 8, LANES)
        return unpack(cap, blocks, where, shift, slot, arrived), near

    level = jnp.sum((needed > jnp.asarray(caps[:-1], jnp.int32)).astype(jnp.int32))
    (windows, edges, heads, tails), near = lax.switch(
        level,
        [functools.partial(exchange, cap) for cap in caps],
        potentials, above1, below1, where, row_offset, slot, source,
    )
    above = passed(tails, 1)
    below = passed(heads, -1)
    return assemble(ratios, windows, edges, above, below, near)


def solution(mesh):
    return jax.shard_map(
        per_device,
        mesh=mesh,
        in_specs=(P("cosmo", "row", None), P("cosmo"), P("cosmo"), P("cosmo")),
        out_specs=(
            P(("cosmo", "row"), None),
            P(None, ("cosmo", "row"), None),
            P(("cosmo", "row"), None),
            P(None, ("cosmo", "row"), None),
        ),
        check_vma=False,
    )
```

```python
import functools

import jax
import jax.numpy as jnp
from jax import lax
from jax.experimental import pallas as pl
from jax.experimental.pallas import tpu as pltpu
from jax.sharding import PartitionSpec as P

RB = 8
LANES = 128
EDGE = 8
STRIDE = 32
CAPS = (18, 20, 21, 22, 23, 24, 26, 30)
C1, C2 = 8.0 / 12.0, 1.0 / 12.0
VMEM = pl.BlockSpec(memory_space=pltpu.VMEM)
SMEM = pl.BlockSpec(memory_space=pltpu.SMEM)


def lanes_of(rows):
    return lax.broadcasted_iota(jnp.int32, (rows, LANES), 1)


def params(mib):
    return pltpu.CompilerParams(vmem_limit_bytes=mib * 2**20)


def tiles_of(cap):
    return 2 * cap + -(-cap // 8)


def first(ahead, behind, ahead2, behind2):
    return C1 * (ahead - behind) - C2 * (ahead2 - behind2)


def second(centre, pairs):
    one, two, three, four = pairs
    return (four - 16.0 * three + 64.0 * two + 16.0 * one - 130.0 * centre) * (1.0 / 144.0)


def rows_of(window):
    def at(k):
        return window[8 + k : 24 + k, :]

    a1, b1, a2, b2 = at(1), at(-1), at(2), at(-2)
    slope = first(a1, b1, a2, b2)
    curve = second(at(0), (a1 + b1, a2 + b2, at(3) + at(-3), at(4) + at(-4)))
    return slope, curve


def slope_rows(window):
    def at(k):
        return window[8 + k : 24 + k, :]

    return first(at(1), at(-1), at(2), at(-2))


def shifted(field, beside, k, lane):
    if k > 0:
        return pltpu.roll(jnp.where(lane < k, beside, field), LANES - k, 1)
    return pltpu.roll(jnp.where(lane >= LANES + k, beside, field), -k, 1)


def columns_of(field, beside, lane):
    def at(k):
        return shifted(field, beside, k, lane)

    a1, b1, a2, b2 = at(1), at(-1), at(2), at(-2)
    slope_c = first(a1, b1, a2, b2)
    curve_cc = second(field, (a1 + b1, a2 + b2, at(3) + at(-3), at(4) + at(-4)))
    return slope_c, curve_cc


def column_slope(field, beside, lane):
    def at(k):
        return shifted(field, beside, k, lane)

    return first(at(1), at(-1), at(2), at(-2))


def near_kernel(blocks, p_ref, up_ref, down_ref, r_ref, c_ref, rr_ref, rc_ref, cc_ref, f_ref):
    lane = lanes_of(16)

    def rows(b, _):
        col = pl.multiple_of(b * LANES, LANES)
        base = pl.multiple_of(b * STRIDE, STRIDE)
        out = pl.multiple_of(b * 16, 16)
        window = f_ref.at[pl.ds(base, STRIDE), :]
        window[4:8, :] = up_ref[:, pl.ds(col, LANES)]
        window[8:24, :] = p_ref[:, pl.ds(col, LANES)]
        window[24:28, :] = down_ref[:, pl.ds(col, LANES)]
        slope, curve = rows_of(window)
        r_ref[pl.ds(out, 16), :] = slope
        rr_ref[pl.ds(out, 16), :] = curve
        return 0

    lax.fori_loop(0, blocks, rows, 0, unroll=8)

    def columns(b, _):
        before = lax.rem(b + (blocks - 1), blocks)
        after = lax.rem(b + 1, blocks)

        def of(i):
            return p_ref[:, pl.ds(pl.multiple_of(i * LANES, LANES), LANES)]

        def slope_of(i):
            return r_ref[pl.ds(pl.multiple_of(i * 16, 16), 16), :]

        far = lane >= LANES // 2
        slope_c, curve_cc = columns_of(of(b), jnp.where(far, of(before), of(after)), lane)
        curve_rc = column_slope(slope_of(b), jnp.where(far, slope_of(before), slope_of(after)), lane)
        out = pl.ds(pl.multiple_of(b * 16, 16), 16)
        c_ref[out, :] = slope_c
        rc_ref[out, :] = curve_rc
        cc_ref[out, :] = curve_cc
        return 0

    lax.fori_loop(0, blocks, columns, 0, unroll=8)


def near_fields(potentials, up, down):
    height, width = potentials.shape[1:]
    blocks = width // LANES
    shape = jax.ShapeDtypeStruct((blocks * 16, LANES), jnp.float32)
    return pl.pallas_call(
        functools.partial(near_kernel, blocks),
        grid=(1,),
        out_shape=(shape,) * 5,
        in_specs=[pl.BlockSpec((None, height, width), lambda i: (0, 0, 0)), VMEM, VMEM],
        out_specs=(VMEM,) * 5,
        scratch_shapes=[pltpu.VMEM((blocks * STRIDE, LANES), jnp.float32)],
        compiler_params=params(16),
        cost_estimate=pl.CostEstimate(flops=60_000_000, bytes_accessed=7_000_000, transcendentals=0),
        name="near_fields",
    )(potentials, up, down)


def index_kernel(blocks, caps, row_ref, col_ref, code_ref, level_ref):
    lane = lax.broadcasted_iota(jnp.int32, (RB, blocks), 1)
    row = row_ref[...]
    alike = lax.broadcasted_iota(jnp.int32, (RB, blocks), 0) == row
    count = alike.astype(jnp.int32)
    step = 1
    while step < blocks:
        count = count + jnp.where(lane >= step, pltpu.roll(count, step, 1), 0)
        step *= 2
    slot = jnp.sum(jnp.where(alike, count - 1, 0), axis=0, keepdims=True)
    source = lane[0:1] + col_ref[...]
    source = jnp.where(source >= blocks, source - blocks, source)
    code_ref[...] = source * 4096 + slot * 8 + row
    needed = jnp.max(count)
    level = jnp.int32(0)
    for cap in caps[:-1]:
        level = level + (needed > cap).astype(jnp.int32)
    level_ref[0] = level


def index_of(row_offset, col_offset, caps):
    blocks = row_offset.shape[0]
    code, level = pl.pallas_call(
        functools.partial(index_kernel, blocks, caps),
        out_shape=(jax.ShapeDtypeStruct((1, blocks), jnp.int32), jax.ShapeDtypeStruct((1,), jnp.int32)),
        in_specs=[VMEM, VMEM],
        out_specs=(VMEM, SMEM),
        name="block_index",
    )(row_offset.reshape(1, blocks), col_offset.reshape(1, blocks))
    return code.reshape(blocks), level[0]


def decoded(code):
    return code >> 12, (code >> 3) & 511, code & 7


def pack_kernel(blocks, cap, here_ref, code_ref, p_ref, out_ref):
    here = here_ref[0]
    tall = tiles_of(cap) * 8
    lane = lanes_of(8)
    far = lane >= LANES // 2

    def block(b, _):
        source, slot, shift = decoded(code_ref[b])
        start = ((here + RB - shift) & (RB - 1)) * tall
        before = jnp.where(source == 0, blocks - 1, source - 1)
        after = jnp.where(source == blocks - 1, 0, source + 1)

        def of(i):
            return p_ref[:, pl.ds(pl.multiple_of(i * LANES, LANES), LANES)]

        out_ref[pl.ds(pl.multiple_of(start + slot * 16, 8), 16), :] = of(source)
        left, right = of(before), of(after)
        place = (slot & 7) * EDGE
        row = pl.ds(pl.multiple_of(start + 16 * cap + (slot >> 3) * 8, 8), 8)
        for half in range(2):
            top = 8 * half
            edge = jnp.where(far, left[top : top + 8], right[top : top + 8])
            spot = place + half * (LANES // 2)
            moved = pltpu.roll(edge, spot + EDGE // 2, 1)
            mask = (lane >= spot) & (lane < spot + EDGE)
            pltpu.store(out_ref.at[row, :], moved, mask=mask)
        return 0

    lax.fori_loop(0, blocks, block, 0, unroll=8)


def pack(cap, here, code, potentials):
    height, width = potentials.shape[1:]
    blocks = width // LANES
    return pl.pallas_call(
        functools.partial(pack_kernel, blocks, cap),
        grid=(1,),
        out_shape=jax.ShapeDtypeStruct((RB * tiles_of(cap) * 8, LANES), jnp.float32),
        in_specs=[SMEM] * 2 + [pl.BlockSpec((None, height, width), lambda i: (1, 0, 0))],
        out_specs=VMEM,
        compiler_params=params(24),
        cost_estimate=pl.CostEstimate(flops=2_000_000, bytes_accessed=3_000_000, transcendentals=0),
        name="pack_blocks",
    )(here, code, potentials)


def unpack_kernel(blocks, cap, here_ref, code_ref, in_ref, w_ref, h_ref, head_ref, tail_ref):
    here = here_ref[0]
    tall = tiles_of(cap) * 8
    lane = lanes_of(8)

    def block(b, _):
        _, slot, shift = decoded(code_ref[b])
        start = ((here + shift) & (RB - 1)) * tall
        tile = in_ref[pl.ds(pl.multiple_of(start + slot * 16, 8), 16), :]
        col = pl.ds(pl.multiple_of(b * LANES, LANES), LANES)
        w_ref[pl.ds(pl.multiple_of(b * 16, 16), 16), :] = tile
        head_ref[:, col] = tile[0:4]
        tail_ref[:, col] = tile[12:16]
        edge = in_ref[pl.ds(pl.multiple_of(start + 16 * cap + (slot >> 3) * 8, 8), 8), :]
        spot = (b & 15) * EDGE
        turn = spot + LANES - (slot & 7) * EDGE
        mask = (lane >= spot) & (lane < spot + EDGE)
        row = pl.multiple_of((b >> 4) * 16, 16)
        pltpu.store(h_ref.at[pl.ds(row, 8), :], pltpu.roll(edge, turn & (LANES - 1), 1), mask=mask)
        half = (turn + LANES // 2) & (LANES - 1)
        pltpu.store(h_ref.at[pl.ds(row + 8, 8), :], pltpu.roll(edge, half, 1), mask=mask)
        return 0

    lax.fori_loop(0, blocks, block, 0, unroll=8)
    for g in range(blocks // 16):
        col = slice((blocks + g) * LANES, (blocks + g + 1) * LANES)
        head_ref[:, col] = h_ref[16 * g : 16 * g + 4, :]
        tail_ref[:, col] = h_ref[16 * g + 12 : 16 * g + 16, :]


def unpack(cap, blocks, here, code, arrived):
    ends = jax.ShapeDtypeStruct((4, (blocks + blocks // 16) * LANES), jnp.float32)
    return pl.pallas_call(
        functools.partial(unpack_kernel, blocks, cap),
        out_shape=(
            jax.ShapeDtypeStruct((blocks * 16, LANES), jnp.float32),
            jax.ShapeDtypeStruct((blocks, LANES), jnp.float32),
            ends,
            ends,
        ),
        in_specs=[SMEM] * 2 + [VMEM],
        out_specs=(VMEM,) * 4,
        compiler_params=params(24),
        cost_estimate=pl.CostEstimate(flops=2_000_000, bytes_accessed=3_000_000, transcendentals=0),
        name="unpack_blocks",
    )(here, code, arrived)


def edge_turn(b):
    return LANES - EDGE // 2 - b * EDGE


def columns_kernel(blocks, w_ref, h_ref, c_ref, cc_ref, g_ref):
    lane = lanes_of(16)

    def spread(i, _):
        edge = h_ref[pl.ds(pl.multiple_of(i * 16, 16), 16), :]
        for k in range(16):
            g_ref[pl.ds(pl.multiple_of(i * 256 + k * 16, 16), 16), :] = pltpu.roll(edge, edge_turn(k), 1)
        return 0

    lax.fori_loop(0, blocks // 16, spread, 0)

    def block(b, _):
        tile = pl.ds(pl.multiple_of(b * 16, 16), 16)
        c_ref[tile, :], cc_ref[tile, :] = columns_of(w_ref[tile, :], g_ref[tile, :], lane)
        return 0

    lax.fori_loop(0, blocks, block, 0, unroll=8)


def far_columns(windows, edges):
    blocks = edges.shape[0]
    return pl.pallas_call(
        functools.partial(columns_kernel, blocks),
        out_shape=(jax.ShapeDtypeStruct(windows.shape, jnp.float32),) * 2,
        in_specs=[VMEM, VMEM],
        out_specs=(VMEM, VMEM),
        scratch_shapes=[pltpu.VMEM(windows.shape, jnp.float32)],
        compiler_params=params(8),
        cost_estimate=pl.CostEstimate(flops=20_000_000, bytes_accessed=3_000_000, transcendentals=0),
        name="far_columns",
    )(windows, edges)


def far_kernel(
    ratio_ref, w_ref, h_ref, up_ref, down_ref, far_c_ref, far_cc_ref, r_ref, c_ref, rr_ref, rc_ref, cc_ref,
    conv_ref, shear_ref, rot_ref, disp_ref, f_ref, e_ref, s_ref,
):
    group = pl.program_id(0)
    blocks = h_ref.shape[0]
    lane = lanes_of(16)
    near_to_two, near_to_source, two_to_source = ratio_ref[0], ratio_ref[1], ratio_ref[2]
    half_one, half_two = 0.5 * near_to_source, 0.5 * two_to_source
    ends = pl.ds(pl.multiple_of((blocks + group) * LANES, LANES), LANES)
    e_ref[4:8, :] = up_ref[:, ends]
    e_ref[8:24, :] = h_ref[pl.ds(pl.multiple_of(group * 16, 16), 16), :]
    e_ref[24:28, :] = down_ref[:, ends]
    s_ref[...] = slope_rows(e_ref)

    def block(i, _):
        b = group * 16 + i
        col = pl.ds(pl.multiple_of(i * LANES, LANES), LANES)
        whole = pl.ds(pl.multiple_of(b * LANES, LANES), LANES)
        tile = pl.ds(pl.multiple_of(b * 16, 16), 16)
        window = f_ref.at[pl.ds(pl.multiple_of(i * STRIDE, STRIDE), STRIDE), :]
        window[4:8, :] = up_ref[:, whole]
        window[8:24, :] = w_ref[tile, :]
        window[24:28, :] = down_ref[:, whole]
        far_r, far_rr = rows_of(window)
        far_rc = column_slope(far_r, pltpu.roll(s_ref[...], edge_turn(i), 1), lane)
        far_cc = far_cc_ref[tile, :]
        near = pl.ds(pl.multiple_of(i * 16, 16), 16)
        near_rr, near_rc, near_cc = rr_ref[near, :], rc_ref[near, :], cc_ref[near, :]
        inner_rr = 1.0 - near_to_two * near_rr
        inner_rc = -near_to_two * near_rc
        inner_cc = 1.0 - near_to_two * near_cc
        chain_rr = far_rr * inner_rr + far_rc * inner_rc
        chain_rc = far_rr * inner_rc + far_rc * inner_cc
        chain_cr = far_rc * inner_rr + far_cc * inner_rc
        chain_cc = far_rc * inner_rc + far_cc * inner_cc
        conv_ref[:, col] = half_one * (near_rr + near_cc) + half_two * (chain_rr + chain_cc)
        shear_ref[0, :, col] = half_one * (near_cc - near_rr) + half_two * (chain_cc - chain_rr)
        shear_ref[1, :, col] = near_to_source * near_rc + half_two * (chain_rc + chain_cr)
        rot_ref[:, col] = half_two * (chain_cr - chain_rc)
        disp_ref[0, :, col] = near_to_source * r_ref[near, :] + two_to_source * far_r
        disp_ref[1, :, col] = near_to_source * c_ref[near, :] + two_to_source * far_c_ref[tile, :]
        return 0

    lax.fori_loop(0, 16, block, 0, unroll=16)


def assemble(ratios, windows, edges, above, below, far, near):
    blocks = edges.shape[0]
    wide = 16 * LANES
    flat = jax.ShapeDtypeStruct((16, blocks * LANES), jnp.float32)
    pair = jax.ShapeDtypeStruct((2, 16, blocks * LANES), jnp.float32)
    flat_spec = pl.BlockSpec((16, wide), lambda i: (0, i))
    pair_spec = pl.BlockSpec((2, 16, wide), lambda i: (0, 0, i))
    return pl.pallas_call(
        far_kernel,
        grid=(blocks // 16,),
        out_shape=(flat, pair, flat, pair),
        in_specs=[SMEM] + [VMEM] * 6 + [pl.BlockSpec((256, LANES), lambda i: (i, 0))] * 5,
        out_specs=(flat_spec, pair_spec, flat_spec, pair_spec),
        scratch_shapes=[
            pltpu.VMEM((16 * STRIDE, LANES), jnp.float32),
            pltpu.VMEM((STRIDE, LANES), jnp.float32),
            pltpu.VMEM((16, LANES), jnp.float32),
        ],
        compiler_params=params(16),
        cost_estimate=pl.CostEstimate(flops=40_000_000, bytes_accessed=6_000_000, transcendentals=0),
        name="far_fields",
    )(ratios, windows, edges, above, below, *far, *near)


def passed(x, by):
    size = lax.axis_size("row")
    return lax.ppermute(x, "row", [(i, (i + by) % size) for i in range(size)])


def near_plane(potentials):
    height = potentials.shape[1]
    above = passed(potentials[0, height - 4 :, :], 1)
    below = passed(potentials[0, :4, :], -1)
    return near_fields(potentials, above, below)


def near_blank(potentials):
    width = potentials.shape[2]
    return (jnp.zeros((width // LANES * 16, LANES), jnp.float32),) * 5


def exchange(cap, groups, potentials, here, code):
    blocks = potentials.shape[2] // LANES
    packed = pack(cap, here, code, potentials).reshape(RB, tiles_of(cap) * 8, LANES)
    arrived = lax.all_to_all(packed, "row", 0, 0, axis_index_groups=groups)
    near = lax.cond(here[0] >= 0, near_plane, near_blank, potentials)
    arrived = arrived.reshape(RB * tiles_of(cap) * 8, LANES)
    return unpack(cap, blocks, here, code, arrived), near


def per_device(potentials, ratios, row_offset, col_offset):
    stride = lax.axis_size("row") // RB
    blocks = potentials.shape[2] // LANES
    caps = tuple(c for c in CAPS if c < blocks) + (blocks,)
    code, level = index_of(row_offset, col_offset, caps)
    here = (lax.axis_index("row") // stride).astype(jnp.int32).reshape(1)
    groups = [[y * stride + j for y in range(RB)] for j in range(stride)]
    (windows, edges, heads, tails), near = lax.switch(
        level,
        [functools.partial(exchange, cap, groups) for cap in caps],
        potentials, here, code,
    )
    above = passed(tails, 1)
    below = passed(heads, -1)
    far = far_columns(windows, edges)
    return assemble(ratios, windows, edges, above, below, far, near)


def solution(mesh):
    return jax.shard_map(
        per_device,
        mesh=mesh,
        in_specs=(P("cosmo", "row", None), P("cosmo"), P("cosmo"), P("cosmo")),
        out_specs=(
            P(("cosmo", "row"), None),
            P(None, ("cosmo", "row"), None),
            P(("cosmo", "row"), None),
            P(None, ("cosmo", "row"), None),
        ),
        check_vma=False,
    )
```

```python
import functools

import jax
import jax.numpy as jnp
from jax import lax
from jax.experimental import pallas as pl
from jax.experimental.pallas import tpu as pltpu
from jax.sharding import PartitionSpec as P

RB = 8
LANES = 128
EDGE = 8
STRIDE = 32
CAPS = (18, 20, 21, 22, 23, 24, 26, 30)
C1, C2 = 8.0 / 12.0, 1.0 / 12.0
VMEM = pl.BlockSpec(memory_space=pltpu.VMEM)
SMEM = pl.BlockSpec(memory_space=pltpu.SMEM)


def lanes_of(rows):
    return lax.broadcasted_iota(jnp.int32, (rows, LANES), 1)


def params(mib):
    return pltpu.CompilerParams(vmem_limit_bytes=mib * 2**20)


def tiles_of(cap):
    return 2 * cap + -(-cap // 8)


def first(ahead, behind, ahead2, behind2):
    return C1 * (ahead - behind) - C2 * (ahead2 - behind2)


def second(centre, pairs):
    one, two, three, four = pairs
    return (four - 16.0 * three + 64.0 * two + 16.0 * one - 130.0 * centre) * (1.0 / 144.0)


def rows_of(window):
    def at(k):
        return window[8 + k : 24 + k, :]

    a1, b1, a2, b2 = at(1), at(-1), at(2), at(-2)
    slope = first(a1, b1, a2, b2)
    curve = second(at(0), (a1 + b1, a2 + b2, at(3) + at(-3), at(4) + at(-4)))
    return slope, curve


def slope_rows(window):
    def at(k):
        return window[8 + k : 24 + k, :]

    return first(at(1), at(-1), at(2), at(-2))


def shifted(field, beside, k, lane):
    if k > 0:
        return pltpu.roll(jnp.where(lane < k, beside, field), LANES - k, 1)
    return pltpu.roll(jnp.where(lane >= LANES + k, beside, field), -k, 1)


def columns_of(field, beside, lane):
    def at(k):
        return shifted(field, beside, k, lane)

    a1, b1, a2, b2 = at(1), at(-1), at(2), at(-2)
    slope_c = first(a1, b1, a2, b2)
    curve_cc = second(field, (a1 + b1, a2 + b2, at(3) + at(-3), at(4) + at(-4)))
    return slope_c, curve_cc


def column_slope(field, beside, lane):
    def at(k):
        return shifted(field, beside, k, lane)

    return first(at(1), at(-1), at(2), at(-2))


def near_kernel(blocks, p_ref, up_ref, down_ref, r_ref, c_ref, rr_ref, rc_ref, cc_ref, f_ref):
    lane = lanes_of(16)

    def rows(b, _):
        col = pl.multiple_of(b * LANES, LANES)
        base = pl.multiple_of(b * STRIDE, STRIDE)
        out = pl.multiple_of(b * 16, 16)
        window = f_ref.at[pl.ds(base, STRIDE), :]
        window[4:8, :] = up_ref[:, pl.ds(col, LANES)]
        window[8:24, :] = p_ref[:, pl.ds(col, LANES)]
        window[24:28, :] = down_ref[:, pl.ds(col, LANES)]
        slope, curve = rows_of(window)
        r_ref[pl.ds(out, 16), :] = slope
        rr_ref[pl.ds(out, 16), :] = curve
        return 0

    lax.fori_loop(0, blocks, rows, 0, unroll=8)

    def columns(b, _):
        before = lax.rem(b + (blocks - 1), blocks)
        after = lax.rem(b + 1, blocks)

        def of(i):
            return p_ref[:, pl.ds(pl.multiple_of(i * LANES, LANES), LANES)]

        def slope_of(i):
            return r_ref[pl.ds(pl.multiple_of(i * 16, 16), 16), :]

        far = lane >= LANES // 2
        slope_c, curve_cc = columns_of(of(b), jnp.where(far, of(before), of(after)), lane)
        curve_rc = column_slope(slope_of(b), jnp.where(far, slope_of(before), slope_of(after)), lane)
        out = pl.ds(pl.multiple_of(b * 16, 16), 16)
        c_ref[out, :] = slope_c
        rc_ref[out, :] = curve_rc
        cc_ref[out, :] = curve_cc
        return 0

    lax.fori_loop(0, blocks, columns, 0, unroll=8)


def near_fields(potentials, up, down):
    height, width = potentials.shape[1:]
    blocks = width // LANES
    shape = jax.ShapeDtypeStruct((blocks * 16, LANES), jnp.float32)
    return pl.pallas_call(
        functools.partial(near_kernel, blocks),
        grid=(1,),
        out_shape=(shape,) * 5,
        in_specs=[pl.BlockSpec((None, height, width), lambda i: (0, 0, 0)), VMEM, VMEM],
        out_specs=(VMEM,) * 5,
        scratch_shapes=[pltpu.VMEM((blocks * STRIDE, LANES), jnp.float32)],
        compiler_params=params(16),
        cost_estimate=pl.CostEstimate(flops=60_000_000, bytes_accessed=7_000_000, transcendentals=0),
        name="near_fields",
    )(potentials, up, down)


def index_kernel(blocks, caps, row_ref, col_ref, code_ref, level_ref):
    lane = lax.broadcasted_iota(jnp.int32, (RB, blocks), 1)
    row = row_ref[...]
    alike = lax.broadcasted_iota(jnp.int32, (RB, blocks), 0) == row
    count = alike.astype(jnp.int32)
    step = 1
    while step < blocks:
        count = count + jnp.where(lane >= step, pltpu.roll(count, step, 1), 0)
        step *= 2
    slot = jnp.sum(jnp.where(alike, count - 1, 0), axis=0, keepdims=True)
    source = lane[0:1] + col_ref[...]
    source = jnp.where(source >= blocks, source - blocks, source)
    code_ref[...] = source * 4096 + slot * 8 + row
    needed = jnp.max(count)
    level = jnp.int32(0)
    for cap in caps[:-1]:
        level = level + (needed > cap).astype(jnp.int32)
    level_ref[0] = level


def index_of(row_offset, col_offset, caps):
    blocks = row_offset.shape[0]
    code, level = pl.pallas_call(
        functools.partial(index_kernel, blocks, caps),
        out_shape=(jax.ShapeDtypeStruct((1, blocks), jnp.int32), jax.ShapeDtypeStruct((1,), jnp.int32)),
        in_specs=[VMEM, VMEM],
        out_specs=(VMEM, SMEM),
        name="block_index",
    )(row_offset.reshape(1, blocks), col_offset.reshape(1, blocks))
    return code.reshape(blocks), level[0]


def decoded(code):
    return code >> 12, (code >> 3) & 511, code & 7


def pack_kernel(blocks, cap, here_ref, code_ref, p_in, out_hbm, p_ref, out_ref, in_sem, out_sem):
    wide = blocks * LANES // 4
    loads = []
    for i in range(4):
        cols = pl.ds(i * wide, wide)
        loads.append(pltpu.make_async_copy(p_in.at[1, :, cols], p_ref.at[:, cols], in_sem.at[i]))
    for copy in loads:
        copy.start()
    here = here_ref[0]
    tall = tiles_of(cap) * 8
    lane = lanes_of(8)
    far = lane >= LANES // 2

    def block(b, _):
        source, slot, shift = decoded(code_ref[b])
        start = ((here + RB - shift) & (RB - 1)) * tall
        before = jnp.where(source == 0, blocks - 1, source - 1)
        after = jnp.where(source == blocks - 1, 0, source + 1)

        def of(i):
            return p_ref[:, pl.ds(pl.multiple_of(i * LANES, LANES), LANES)]

        out_ref[pl.ds(pl.multiple_of(start + slot * 16, 8), 16), :] = of(source)
        left, right = of(before), of(after)
        place = (slot & 7) * EDGE
        row = pl.ds(pl.multiple_of(start + 16 * cap + (slot >> 3) * 8, 8), 8)
        for half in range(2):
            top = 8 * half
            edge = jnp.where(far, left[top : top + 8], right[top : top + 8])
            spot = place + half * (LANES // 2)
            moved = pltpu.roll(edge, spot + EDGE // 2, 1)
            mask = (lane >= spot) & (lane < spot + EDGE)
            pltpu.store(out_ref.at[row, :], moved, mask=mask)
        return 0

    for copy in loads:
        copy.wait()
    lax.fori_loop(0, blocks, block, 0, unroll=16)
    stores = []
    for i in range(RB):
        rows = pl.ds(i * tall, tall)
        stores.append(pltpu.make_async_copy(out_ref.at[rows, :], out_hbm.at[rows, :], out_sem.at[i]))
    for copy in stores:
        copy.start()
    for copy in stores:
        copy.wait()


def pack(cap, here, code, potentials):
    height, width = potentials.shape[1:]
    blocks = width // LANES
    shape = (RB * tiles_of(cap) * 8, LANES)
    return pl.pallas_call(
        functools.partial(pack_kernel, blocks, cap),
        out_shape=jax.ShapeDtypeStruct(shape, jnp.float32),
        in_specs=[SMEM] * 2 + [pl.BlockSpec(memory_space=pl.ANY)],
        out_specs=pl.BlockSpec(memory_space=pl.ANY),
        scratch_shapes=[
            pltpu.VMEM((height, width), jnp.float32),
            pltpu.VMEM(shape, jnp.float32),
            pltpu.SemaphoreType.DMA((4,)),
            pltpu.SemaphoreType.DMA((RB,)),
        ],
        compiler_params=params(24),
        cost_estimate=pl.CostEstimate(flops=2_000_000, bytes_accessed=3_000_000, transcendentals=0),
        name="pack_blocks",
    )(here, code, potentials)


def unpack_kernel(blocks, cap, here_ref, code_ref, in_ref, w_ref, h_ref, head_ref, tail_ref):
    here = here_ref[0]
    tall = tiles_of(cap) * 8
    lane = lanes_of(8)

    def block(b, _):
        _, slot, shift = decoded(code_ref[b])
        start = ((here + shift) & (RB - 1)) * tall
        tile = in_ref[pl.ds(pl.multiple_of(start + slot * 16, 8), 16), :]
        col = pl.ds(pl.multiple_of(b * LANES, LANES), LANES)
        w_ref[pl.ds(pl.multiple_of(b * 16, 16), 16), :] = tile
        head_ref[:, col] = tile[0:4]
        tail_ref[:, col] = tile[12:16]
        edge = in_ref[pl.ds(pl.multiple_of(start + 16 * cap + (slot >> 3) * 8, 8), 8), :]
        spot = (b & 15) * EDGE
        turn = spot + LANES - (slot & 7) * EDGE
        mask = (lane >= spot) & (lane < spot + EDGE)
        row = pl.multiple_of((b >> 4) * 16, 16)
        pltpu.store(h_ref.at[pl.ds(row, 8), :], pltpu.roll(edge, turn & (LANES - 1), 1), mask=mask)
        half = (turn + LANES // 2) & (LANES - 1)
        pltpu.store(h_ref.at[pl.ds(row + 8, 8), :], pltpu.roll(edge, half, 1), mask=mask)
        return 0

    lax.fori_loop(0, blocks, block, 0, unroll=16)
    for g in range(blocks // 16):
        col = slice((blocks + g) * LANES, (blocks + g + 1) * LANES)
        head_ref[:, col] = h_ref[16 * g : 16 * g + 4, :]
        tail_ref[:, col] = h_ref[16 * g + 12 : 16 * g + 16, :]


def unpack(cap, blocks, here, code, arrived):
    ends = jax.ShapeDtypeStruct((4, (blocks + blocks // 16) * LANES), jnp.float32)
    return pl.pallas_call(
        functools.partial(unpack_kernel, blocks, cap),
        out_shape=(
            jax.ShapeDtypeStruct((blocks * 16, LANES), jnp.float32),
            jax.ShapeDtypeStruct((blocks, LANES), jnp.float32),
            ends,
            ends,
        ),
        in_specs=[SMEM] * 2 + [VMEM],
        out_specs=(VMEM,) * 4,
        compiler_params=params(24),
        cost_estimate=pl.CostEstimate(flops=2_000_000, bytes_accessed=3_000_000, transcendentals=0),
        name="unpack_blocks",
    )(here, code, arrived)


def edge_turn(b):
    return LANES - EDGE // 2 - b * EDGE


def columns_kernel(blocks, h_ref, w_in, n0, n1, n2, n3, n4, c_ref, cc_ref, w_ref, m0, m1, m2, m3, m4, g_ref, w_sem, sem):
    lane = lanes_of(16)
    quarter = blocks * 4

    def part(i):
        rows = pl.ds(i * quarter, quarter)
        return pltpu.make_async_copy(w_in.at[rows, :], w_ref.at[rows, :], w_sem.at[i])

    near = [pltpu.make_async_copy(n, m, sem.at[i]) for i, (n, m) in enumerate(zip((n0, n1, n2, n3, n4), (m0, m1, m2, m3, m4)))]
    for i in range(4):
        part(i).start()

    def spread(i, _):
        edge = h_ref[pl.ds(pl.multiple_of(i * 16, 16), 16), :]
        for k in range(16):
            g_ref[pl.ds(pl.multiple_of(i * 256 + k * 16, 16), 16), :] = pltpu.roll(edge, edge_turn(k), 1)
        return 0

    lax.fori_loop(0, blocks // 16, spread, 0)
    for i in range(4):
        part(i).wait()
    for copy in near:
        copy.start()

    def block(b, _):
        tile = pl.ds(pl.multiple_of(b * 16, 16), 16)
        c_ref[tile, :], cc_ref[tile, :] = columns_of(w_ref[tile, :], g_ref[tile, :], lane)
        return 0

    lax.fori_loop(0, blocks, block, 0, unroll=8)
    for copy in near:
        copy.wait()


def far_columns(windows, edges, near):
    blocks = edges.shape[0]
    anywhere = pl.BlockSpec(memory_space=pl.ANY)
    out = pl.pallas_call(
        functools.partial(columns_kernel, blocks),
        out_shape=(jax.ShapeDtypeStruct(windows.shape, jnp.float32),) * 8,
        in_specs=[VMEM] + [anywhere] * 6,
        out_specs=(VMEM,) * 8,
        scratch_shapes=[
            pltpu.VMEM(windows.shape, jnp.float32),
            pltpu.SemaphoreType.DMA((4,)),
            pltpu.SemaphoreType.DMA((5,)),
        ],
        compiler_params=params(16),
        cost_estimate=pl.CostEstimate(flops=20_000_000, bytes_accessed=3_000_000, transcendentals=0),
        name="far_columns",
    )(edges, windows, *near)
    return out[:2], out[2], out[3:]


def far_kernel(
    ratio_ref, w_ref, h_ref, up_ref, down_ref, far_c_ref, far_cc_ref, r_ref, c_ref, rr_ref, rc_ref, cc_ref,
    conv_ref, shear_ref, rot_ref, disp_ref, f_ref, e_ref, s_ref,
):
    group = pl.program_id(0)
    blocks = h_ref.shape[0]
    lane = lanes_of(16)
    near_to_two, near_to_source, two_to_source = ratio_ref[0], ratio_ref[1], ratio_ref[2]
    half_one, half_two = 0.5 * near_to_source, 0.5 * two_to_source
    ends = pl.ds(pl.multiple_of((blocks + group) * LANES, LANES), LANES)
    e_ref[4:8, :] = up_ref[:, ends]
    e_ref[8:24, :] = h_ref[pl.ds(pl.multiple_of(group * 16, 16), 16), :]
    e_ref[24:28, :] = down_ref[:, ends]
    s_ref[...] = slope_rows(e_ref)

    def block(i, _):
        b = group * 16 + i
        col = pl.ds(pl.multiple_of(i * LANES, LANES), LANES)
        whole = pl.ds(pl.multiple_of(b * LANES, LANES), LANES)
        tile = pl.ds(pl.multiple_of(b * 16, 16), 16)
        window = f_ref.at[pl.ds(pl.multiple_of(i * STRIDE, STRIDE), STRIDE), :]
        window[4:8, :] = up_ref[:, whole]
        window[8:24, :] = w_ref[tile, :]
        window[24:28, :] = down_ref[:, whole]
        far_r, far_rr = rows_of(window)
        far_rc = column_slope(far_r, pltpu.roll(s_ref[...], edge_turn(i), 1), lane)
        far_cc = far_cc_ref[tile, :]
        near_rr, near_rc, near_cc = rr_ref[tile, :], rc_ref[tile, :], cc_ref[tile, :]
        inner_rr = 1.0 - near_to_two * near_rr
        inner_rc = -near_to_two * near_rc
        inner_cc = 1.0 - near_to_two * near_cc
        chain_rr = far_rr * inner_rr + far_rc * inner_rc
        chain_rc = far_rr * inner_rc + far_rc * inner_cc
        chain_cr = far_rc * inner_rr + far_cc * inner_rc
        chain_cc = far_rc * inner_rc + far_cc * inner_cc
        conv_ref[:, col] = half_one * (near_rr + near_cc) + half_two * (chain_rr + chain_cc)
        shear_ref[0, :, col] = half_one * (near_cc - near_rr) + half_two * (chain_cc - chain_rr)
        shear_ref[1, :, col] = near_to_source * near_rc + half_two * (chain_rc + chain_cr)
        rot_ref[:, col] = half_two * (chain_cr - chain_rc)
        disp_ref[0, :, col] = near_to_source * r_ref[tile, :] + two_to_source * far_r
        disp_ref[1, :, col] = near_to_source * c_ref[tile, :] + two_to_source * far_c_ref[tile, :]
        return 0

    lax.fori_loop(0, 16, block, 0, unroll=16)


def assemble(ratios, windows, edges, above, below, far, near):
    blocks = edges.shape[0]
    wide = 16 * LANES
    flat = jax.ShapeDtypeStruct((16, blocks * LANES), jnp.float32)
    pair = jax.ShapeDtypeStruct((2, 16, blocks * LANES), jnp.float32)
    flat_spec = pl.BlockSpec((16, wide), lambda i: (0, i))
    pair_spec = pl.BlockSpec((2, 16, wide), lambda i: (0, 0, i))
    return pl.pallas_call(
        far_kernel,
        grid=(blocks // 16,),
        out_shape=(flat, pair, flat, pair),
        in_specs=[SMEM] + [VMEM] * 11,
        out_specs=(flat_spec, pair_spec, flat_spec, pair_spec),
        scratch_shapes=[
            pltpu.VMEM((16 * STRIDE, LANES), jnp.float32),
            pltpu.VMEM((STRIDE, LANES), jnp.float32),
            pltpu.VMEM((16, LANES), jnp.float32),
        ],
        compiler_params=params(16),
        cost_estimate=pl.CostEstimate(flops=40_000_000, bytes_accessed=6_000_000, transcendentals=0),
        name="far_fields",
    )(ratios, windows, edges, above, below, *far, *near)


def passed(x, by):
    size = lax.axis_size("row")
    return lax.ppermute(x, "row", [(i, (i + by) % size) for i in range(size)])


def near_plane(potentials):
    height = potentials.shape[1]
    above = passed(potentials[0, height - 4 :, :], 1)
    below = passed(potentials[0, :4, :], -1)
    return near_fields(potentials, above, below)


def near_blank(potentials):
    width = potentials.shape[2]
    return (jnp.zeros((width // LANES * 16, LANES), jnp.float32),) * 5


def exchange(cap, groups, potentials, here, code):
    blocks = potentials.shape[2] // LANES
    packed = pack(cap, here, code, potentials).reshape(RB, tiles_of(cap) * 8, LANES)
    arrived = lax.all_to_all(packed, "row", 0, 0, axis_index_groups=groups)
    near = lax.cond(here[0] >= 0, near_plane, near_blank, potentials)
    arrived = arrived.reshape(RB * tiles_of(cap) * 8, LANES)
    return unpack(cap, blocks, here, code, arrived), near


def per_device(potentials, ratios, row_offset, col_offset):
    stride = lax.axis_size("row") // RB
    blocks = potentials.shape[2] // LANES
    caps = tuple(c for c in CAPS if c < blocks) + (blocks,)
    code, level = index_of(row_offset, col_offset, caps)
    here = (lax.axis_index("row") // stride).astype(jnp.int32).reshape(1)
    groups = [[y * stride + j for y in range(RB)] for j in range(stride)]
    (windows, edges, heads, tails), near = lax.switch(
        level,
        [functools.partial(exchange, cap, groups) for cap in caps],
        potentials, here, code,
    )
    above = passed(tails, 1)
    below = passed(heads, -1)
    far, windows, near = far_columns(windows, edges, near)
    return assemble(ratios, windows, edges, above, below, far, near)


def solution(mesh):
    return jax.shard_map(
        per_device,
        mesh=mesh,
        in_specs=(P("cosmo", "row", None), P("cosmo"), P("cosmo"), P("cosmo")),
        out_specs=(
            P(("cosmo", "row"), None),
            P(None, ("cosmo", "row"), None),
            P(("cosmo", "row"), None),
            P(None, ("cosmo", "row"), None),
        ),
        check_vma=False,
    )
```

```python
import functools

import jax
import jax.numpy as jnp
from jax import lax
from jax.experimental import pallas as pl
from jax.experimental.pallas import tpu as pltpu
from jax.sharding import PartitionSpec as P

RB = 8
LANES = 128
EDGE = 8
STRIDE = 32
CAPS = (21, 22, 23, 24, 25, 26, 28, 32)
C1, C2 = 8.0 / 12.0, 1.0 / 12.0
VMEM = pl.BlockSpec(memory_space=pltpu.VMEM)
SMEM = pl.BlockSpec(memory_space=pltpu.SMEM)


def lanes_of(rows):
    return lax.broadcasted_iota(jnp.int32, (rows, LANES), 1)


def params(mib):
    return pltpu.CompilerParams(vmem_limit_bytes=mib * 2**20)


def tiles_of(cap):
    return 2 * cap + -(-cap // 8)


def first(ahead, behind, ahead2, behind2):
    return C1 * (ahead - behind) - C2 * (ahead2 - behind2)


def second(centre, pairs):
    one, two, three, four = pairs
    return (four - 16.0 * three + 64.0 * two + 16.0 * one - 130.0 * centre) * (1.0 / 144.0)


def rows_of(window):
    def at(k):
        return window[8 + k : 24 + k, :]

    a1, b1, a2, b2 = at(1), at(-1), at(2), at(-2)
    slope = first(a1, b1, a2, b2)
    curve = second(at(0), (a1 + b1, a2 + b2, at(3) + at(-3), at(4) + at(-4)))
    return slope, curve


def slope_rows(window):
    def at(k):
        return window[8 + k : 24 + k, :]

    return first(at(1), at(-1), at(2), at(-2))


def shifted(field, beside, k, lane):
    if k > 0:
        return pltpu.roll(jnp.where(lane < k, beside, field), LANES - k, 1)
    return pltpu.roll(jnp.where(lane >= LANES + k, beside, field), -k, 1)


def columns_of(field, beside, lane):
    def at(k):
        return shifted(field, beside, k, lane)

    a1, b1, a2, b2 = at(1), at(-1), at(2), at(-2)
    slope_c = first(a1, b1, a2, b2)
    curve_cc = second(field, (a1 + b1, a2 + b2, at(3) + at(-3), at(4) + at(-4)))
    return slope_c, curve_cc


def column_slope(field, beside, lane):
    def at(k):
        return shifted(field, beside, k, lane)

    return first(at(1), at(-1), at(2), at(-2))


def near_kernel(blocks, p_ref, up_ref, down_ref, r_ref, c_ref, rr_ref, rc_ref, cc_ref, f_ref):
    lane = lanes_of(16)

    def rows(b, _):
        col = pl.multiple_of(b * LANES, LANES)
        base = pl.multiple_of(b * STRIDE, STRIDE)
        out = pl.multiple_of(b * 16, 16)
        window = f_ref.at[pl.ds(base, STRIDE), :]
        window[4:8, :] = up_ref[:, pl.ds(col, LANES)]
        window[8:24, :] = p_ref[:, pl.ds(col, LANES)]
        window[24:28, :] = down_ref[:, pl.ds(col, LANES)]
        slope, curve = rows_of(window)
        r_ref[pl.ds(out, 16), :] = slope
        rr_ref[pl.ds(out, 16), :] = curve
        return 0

    lax.fori_loop(0, blocks, rows, 0, unroll=8)

    def columns(b, _):
        before = lax.rem(b + (blocks - 1), blocks)
        after = lax.rem(b + 1, blocks)

        def of(i):
            return p_ref[:, pl.ds(pl.multiple_of(i * LANES, LANES), LANES)]

        def slope_of(i):
            return r_ref[pl.ds(pl.multiple_of(i * 16, 16), 16), :]

        far = lane >= LANES // 2
        slope_c, curve_cc = columns_of(of(b), jnp.where(far, of(before), of(after)), lane)
        curve_rc = column_slope(slope_of(b), jnp.where(far, slope_of(before), slope_of(after)), lane)
        out = pl.ds(pl.multiple_of(b * 16, 16), 16)
        c_ref[out, :] = slope_c
        rc_ref[out, :] = curve_rc
        cc_ref[out, :] = curve_cc
        return 0

    lax.fori_loop(0, blocks, columns, 0, unroll=8)


def near_fields(potentials, up, down):
    height, width = potentials.shape[1:]
    blocks = width // LANES
    shape = jax.ShapeDtypeStruct((blocks * 16, LANES), jnp.float32)
    return pl.pallas_call(
        functools.partial(near_kernel, blocks),
        grid=(1,),
        out_shape=(shape,) * 5,
        in_specs=[pl.BlockSpec((None, height, width), lambda i: (0, 0, 0)), VMEM, VMEM],
        out_specs=(VMEM,) * 5,
        scratch_shapes=[pltpu.VMEM((blocks * STRIDE, LANES), jnp.float32)],
        compiler_params=params(16),
        cost_estimate=pl.CostEstimate(flops=60_000_000, bytes_accessed=7_000_000, transcendentals=0),
        name="near_fields",
    )(potentials, up, down)


def index_kernel(blocks, caps, row_ref, col_ref, code_ref, level_ref):
    lane = lax.broadcasted_iota(jnp.int32, (RB, blocks), 1)
    row = row_ref[...]
    alike = lax.broadcasted_iota(jnp.int32, (RB, blocks), 0) == row
    square = (blocks, blocks)
    upto = lax.broadcasted_iota(jnp.int32, square, 0) <= lax.broadcasted_iota(jnp.int32, square, 1)
    count = jnp.dot(alike.astype(jnp.float32), upto.astype(jnp.float32), preferred_element_type=jnp.float32)
    count = count.astype(jnp.int32)
    slot = jnp.sum(jnp.where(alike, count - 1, 0), axis=0, keepdims=True)
    source = lane[0:1] + col_ref[...]
    source = jnp.where(source >= blocks, source - blocks, source)
    code_ref[...] = source * 4096 + slot * 8 + row
    needed = jnp.max(count)
    level = jnp.int32(0)
    for cap in caps[:-1]:
        level = level + (needed > cap).astype(jnp.int32)
    level_ref[0] = level


def index_of(row_offset, col_offset, caps):
    blocks = row_offset.shape[0]
    code, level = pl.pallas_call(
        functools.partial(index_kernel, blocks, caps),
        out_shape=(jax.ShapeDtypeStruct((1, blocks), jnp.int32), jax.ShapeDtypeStruct((1,), jnp.int32)),
        in_specs=[VMEM, VMEM],
        out_specs=(VMEM, SMEM),
        name="block_index",
    )(row_offset.reshape(1, blocks), col_offset.reshape(1, blocks))
    return code.reshape(blocks), level[0]


def decoded(code):
    return code >> 12, (code >> 3) & 511, code & 7


def pack_kernel(blocks, cap, here_ref, code_ref, p_in, out_hbm, p_ref, out_ref, in_sem, out_sem):
    wide = blocks * LANES // 4
    loads = []
    for i in range(4):
        cols = pl.ds(i * wide, wide)
        loads.append(pltpu.make_async_copy(p_in.at[1, :, cols], p_ref.at[:, cols], in_sem.at[i]))
    for copy in loads:
        copy.start()
    here = here_ref[0]
    tall = tiles_of(cap) * 8
    lane = lanes_of(8)
    far = lane >= LANES // 2

    def block(b, _):
        source, slot, shift = decoded(code_ref[b])
        start = ((here + RB - shift) & (RB - 1)) * tall
        before = jnp.where(source == 0, blocks - 1, source - 1)
        after = jnp.where(source == blocks - 1, 0, source + 1)

        def of(i):
            return p_ref[:, pl.ds(pl.multiple_of(i * LANES, LANES), LANES)]

        out_ref[pl.ds(pl.multiple_of(start + slot * 16, 8), 16), :] = of(source)
        left, right = of(before), of(after)
        place = (slot & 7) * EDGE
        row = pl.ds(pl.multiple_of(start + 16 * cap + (slot >> 3) * 8, 8), 8)
        for half in range(2):
            top = 8 * half
            edge = jnp.where(far, left[top : top + 8], right[top : top + 8])
            spot = place + half * (LANES // 2)
            moved = pltpu.roll(edge, spot + EDGE // 2, 1)
            mask = (lane >= spot) & (lane < spot + EDGE)
            pltpu.store(out_ref.at[row, :], moved, mask=mask)
        return 0

    for copy in loads:
        copy.wait()
    lax.fori_loop(0, blocks, block, 0, unroll=16)
    stores = []
    for i in range(RB):
        rows = pl.ds(i * tall, tall)
        stores.append(pltpu.make_async_copy(out_ref.at[rows, :], out_hbm.at[rows, :], out_sem.at[i]))
    for copy in stores:
        copy.start()
    for copy in stores:
        copy.wait()


def pack(cap, here, code, potentials):
    height, width = potentials.shape[1:]
    blocks = width // LANES
    shape = (RB * tiles_of(cap) * 8, LANES)
    return pl.pallas_call(
        functools.partial(pack_kernel, blocks, cap),
        out_shape=jax.ShapeDtypeStruct(shape, jnp.float32),
        in_specs=[SMEM] * 2 + [pl.BlockSpec(memory_space=pl.ANY)],
        out_specs=pl.BlockSpec(memory_space=pl.ANY),
        scratch_shapes=[
            pltpu.VMEM((height, width), jnp.float32),
            pltpu.VMEM(shape, jnp.float32),
            pltpu.SemaphoreType.DMA((4,)),
            pltpu.SemaphoreType.DMA((RB,)),
        ],
        compiler_params=params(24),
        cost_estimate=pl.CostEstimate(flops=2_000_000, bytes_accessed=3_000_000, transcendentals=0),
        name="pack_blocks",
    )(here, code, potentials)


def unpack_kernel(blocks, cap, here_ref, code_ref, in_ref, w_ref, h_ref, head_ref, tail_ref):
    here = here_ref[0]
    tall = tiles_of(cap) * 8
    lane = lanes_of(8)

    def block(b, _):
        _, slot, shift = decoded(code_ref[b])
        start = ((here + shift) & (RB - 1)) * tall
        tile = in_ref[pl.ds(pl.multiple_of(start + slot * 16, 8), 16), :]
        col = pl.ds(pl.multiple_of(b * LANES, LANES), LANES)
        w_ref[pl.ds(pl.multiple_of(b * 16, 16), 16), :] = tile
        head_ref[:, col] = tile[0:4]
        tail_ref[:, col] = tile[12:16]
        edge = in_ref[pl.ds(pl.multiple_of(start + 16 * cap + (slot >> 3) * 8, 8), 8), :]
        spot = (b & 15) * EDGE
        turn = spot + LANES - (slot & 7) * EDGE
        mask = (lane >= spot) & (lane < spot + EDGE)
        row = pl.multiple_of((b >> 4) * 16, 16)
        pltpu.store(h_ref.at[pl.ds(row, 8), :], pltpu.roll(edge, turn & (LANES - 1), 1), mask=mask)
        half = (turn + LANES // 2) & (LANES - 1)
        pltpu.store(h_ref.at[pl.ds(row + 8, 8), :], pltpu.roll(edge, half, 1), mask=mask)
        return 0

    lax.fori_loop(0, blocks, block, 0, unroll=16)
    for g in range(blocks // 16):
        col = slice((blocks + g) * LANES, (blocks + g + 1) * LANES)
        head_ref[:, col] = h_ref[16 * g : 16 * g + 4, :]
        tail_ref[:, col] = h_ref[16 * g + 12 : 16 * g + 16, :]


def unpack(cap, blocks, here, code, arrived):
    ends = jax.ShapeDtypeStruct((4, (blocks + blocks // 16) * LANES), jnp.float32)
    return pl.pallas_call(
        functools.partial(unpack_kernel, blocks, cap),
        out_shape=(
            jax.ShapeDtypeStruct((blocks * 16, LANES), jnp.float32),
            jax.ShapeDtypeStruct((blocks, LANES), jnp.float32),
            ends,
            ends,
        ),
        in_specs=[SMEM] * 2 + [VMEM],
        out_specs=(VMEM,) * 4,
        compiler_params=params(24),
        cost_estimate=pl.CostEstimate(flops=2_000_000, bytes_accessed=3_000_000, transcendentals=0),
        name="unpack_blocks",
    )(here, code, arrived)


def edge_turn(b):
    return LANES - EDGE // 2 - b * EDGE


def columns_kernel(blocks, h_ref, w_in, n0, n1, n2, n3, n4, c_ref, cc_ref, w_ref, m0, m1, m2, m3, m4, g_ref, w_sem, sem):
    lane = lanes_of(16)
    quarter = blocks * 4

    def part(i):
        rows = pl.ds(i * quarter, quarter)
        return pltpu.make_async_copy(w_in.at[rows, :], w_ref.at[rows, :], w_sem.at[i])

    near = [pltpu.make_async_copy(n, m, sem.at[i]) for i, (n, m) in enumerate(zip((n0, n1, n2, n3, n4), (m0, m1, m2, m3, m4)))]
    for i in range(4):
        part(i).start()

    def spread(i, _):
        edge = h_ref[pl.ds(pl.multiple_of(i * 16, 16), 16), :]
        for k in range(16):
            g_ref[pl.ds(pl.multiple_of(i * 256 + k * 16, 16), 16), :] = pltpu.roll(edge, edge_turn(k), 1)
        return 0

    lax.fori_loop(0, blocks // 16, spread, 0)
    for i in range(4):
        part(i).wait()
    for copy in near:
        copy.start()

    def block(b, _):
        tile = pl.ds(pl.multiple_of(b * 16, 16), 16)
        c_ref[tile, :], cc_ref[tile, :] = columns_of(w_ref[tile, :], g_ref[tile, :], lane)
        return 0

    lax.fori_loop(0, blocks, block, 0, unroll=8)
    for copy in near:
        copy.wait()


def far_columns(windows, edges, near):
    blocks = edges.shape[0]
    anywhere = pl.BlockSpec(memory_space=pl.ANY)
    out = pl.pallas_call(
        functools.partial(columns_kernel, blocks),
        out_shape=(jax.ShapeDtypeStruct(windows.shape, jnp.float32),) * 8,
        in_specs=[VMEM] + [anywhere] * 6,
        out_specs=(VMEM,) * 8,
        scratch_shapes=[
            pltpu.VMEM(windows.shape, jnp.float32),
            pltpu.SemaphoreType.DMA((4,)),
            pltpu.SemaphoreType.DMA((5,)),
        ],
        compiler_params=params(16),
        cost_estimate=pl.CostEstimate(flops=20_000_000, bytes_accessed=3_000_000, transcendentals=0),
        name="far_columns",
    )(edges, windows, *near)
    return out[:2], out[2], out[3:]


def far_kernel(
    ratio_ref, w_ref, h_ref, up_ref, down_ref, far_c_ref, far_cc_ref, r_ref, c_ref, rr_ref, rc_ref, cc_ref,
    conv_out, shear_out, rot_out, disp_out, conv_ref, shear_ref, rot_ref, disp_ref, f_ref, e_ref, s_ref, sem,
):
    blocks = h_ref.shape[0]
    lane = lanes_of(16)
    near_to_two, near_to_source, two_to_source = ratio_ref[0], ratio_ref[1], ratio_ref[2]
    half_one, half_two = 0.5 * near_to_source, 0.5 * two_to_source
    refs = ((conv_ref, conv_out), (shear_ref, shear_out), (rot_ref, rot_out), (disp_ref, disp_out))

    def copies(group):
        cols = pl.ds(pl.multiple_of(group * 16 * LANES, 16 * LANES), 16 * LANES)
        return [
            pltpu.make_async_copy(ref.at[..., cols], out.at[..., cols], sem.at[k, group]) for k, (ref, out) in enumerate(refs)
        ]

    def columns(group, _):
        ends = pl.ds(pl.multiple_of((blocks + group) * LANES, LANES), LANES)
        e_ref[4:8, :] = up_ref[:, ends]
        e_ref[8:24, :] = h_ref[pl.ds(pl.multiple_of(group * 16, 16), 16), :]
        e_ref[24:28, :] = down_ref[:, ends]
        s_ref[...] = slope_rows(e_ref)

        def block(i, _):
            b = group * 16 + i
            col = pl.ds(pl.multiple_of(b * LANES, LANES), LANES)
            tile = pl.ds(pl.multiple_of(b * 16, 16), 16)
            window = f_ref.at[pl.ds(pl.multiple_of(i * STRIDE, STRIDE), STRIDE), :]
            window[4:8, :] = up_ref[:, col]
            window[8:24, :] = w_ref[tile, :]
            window[24:28, :] = down_ref[:, col]
            far_r, far_rr = rows_of(window)
            far_rc = column_slope(far_r, pltpu.roll(s_ref[...], edge_turn(i), 1), lane)
            far_cc = far_cc_ref[tile, :]
            near_rr, near_rc, near_cc = rr_ref[tile, :], rc_ref[tile, :], cc_ref[tile, :]
            inner_rr = 1.0 - near_to_two * near_rr
            inner_rc = -near_to_two * near_rc
            inner_cc = 1.0 - near_to_two * near_cc
            chain_rr = far_rr * inner_rr + far_rc * inner_rc
            chain_rc = far_rr * inner_rc + far_rc * inner_cc
            chain_cr = far_rc * inner_rr + far_cc * inner_rc
            chain_cc = far_rc * inner_rc + far_cc * inner_cc
            conv_ref[:, col] = half_one * (near_rr + near_cc) + half_two * (chain_rr + chain_cc)
            shear_ref[0, :, col] = half_one * (near_cc - near_rr) + half_two * (chain_cc - chain_rr)
            shear_ref[1, :, col] = near_to_source * near_rc + half_two * (chain_rc + chain_cr)
            rot_ref[:, col] = half_two * (chain_cr - chain_rc)
            disp_ref[0, :, col] = near_to_source * r_ref[tile, :] + two_to_source * far_r
            disp_ref[1, :, col] = near_to_source * c_ref[tile, :] + two_to_source * far_c_ref[tile, :]
            return 0

        lax.fori_loop(0, 16, block, 0, unroll=16)
        for copy in copies(group):
            copy.start()
        return 0

    lax.fori_loop(0, blocks // 16, columns, 0)

    def finish(group, _):
        for copy in copies(group):
            copy.wait()
        return 0

    lax.fori_loop(0, blocks // 16, finish, 0)


def assemble(ratios, windows, edges, above, below, far, near):
    blocks = edges.shape[0]
    flat = jax.ShapeDtypeStruct((16, blocks * LANES), jnp.float32)
    pair = jax.ShapeDtypeStruct((2, 16, blocks * LANES), jnp.float32)
    outs = (flat, pair, flat, pair)
    return pl.pallas_call(
        far_kernel,
        out_shape=outs,
        in_specs=[SMEM] + [VMEM] * 11,
        out_specs=(pl.BlockSpec(memory_space=pl.ANY),) * 4,
        scratch_shapes=[pltpu.VMEM(o.shape, o.dtype) for o in outs]
        + [
            pltpu.VMEM((16 * STRIDE, LANES), jnp.float32),
            pltpu.VMEM((STRIDE, LANES), jnp.float32),
            pltpu.VMEM((16, LANES), jnp.float32),
            pltpu.SemaphoreType.DMA((4, blocks // 16)),
        ],
        compiler_params=params(16),
        cost_estimate=pl.CostEstimate(flops=40_000_000, bytes_accessed=6_000_000, transcendentals=0),
        name="far_fields",
    )(ratios, windows, edges, above, below, *far, *near)


def passed(x, by):
    size = lax.axis_size("row")
    return lax.ppermute(x, "row", [(i, (i + by) % size) for i in range(size)])


def near_plane(potentials):
    height = potentials.shape[1]
    above = passed(potentials[0, height - 4 :, :], 1)
    below = passed(potentials[0, :4, :], -1)
    return near_fields(potentials, above, below)


def near_blank(potentials):
    width = potentials.shape[2]
    return (jnp.zeros((width // LANES * 16, LANES), jnp.float32),) * 5


def exchange(cap, groups, potentials, here, code):
    blocks = potentials.shape[2] // LANES
    packed = pack(cap, here, code, potentials).reshape(RB, tiles_of(cap) * 8, LANES)
    arrived = lax.all_to_all(packed, "row", 0, 0, axis_index_groups=groups)
    near = lax.cond(here[0] >= 0, near_plane, near_blank, potentials)
    arrived = arrived.reshape(RB * tiles_of(cap) * 8, LANES)
    return unpack(cap, blocks, here, code, arrived), near


def per_device(potentials, ratios, row_offset, col_offset):
    stride = lax.axis_size("row") // RB
    blocks = potentials.shape[2] // LANES
    caps = tuple(c for c in CAPS if c < blocks) + (blocks,)
    code, level = index_of(row_offset, col_offset, caps)
    here = (lax.axis_index("row") // stride).astype(jnp.int32).reshape(1)
    groups = [[y * stride + j for y in range(RB)] for j in range(stride)]
    (windows, edges, heads, tails), near = lax.switch(
        level,
        [functools.partial(exchange, cap, groups) for cap in caps],
        potentials, here, code,
    )
    above = passed(tails, 1)
    below = passed(heads, -1)
    far, windows, near = far_columns(windows, edges, near)
    return assemble(ratios, windows, edges, above, below, far, near)


def solution(mesh):
    return jax.shard_map(
        per_device,
        mesh=mesh,
        in_specs=(P("cosmo", "row", None), P("cosmo"), P("cosmo"), P("cosmo")),
        out_specs=(
            P(("cosmo", "row"), None),
            P(None, ("cosmo", "row"), None),
            P(("cosmo", "row"), None),
            P(None, ("cosmo", "row"), None),
        ),
        check_vma=False,
    )
```

```python
import functools

import jax
import jax.numpy as jnp
from jax import lax
from jax.experimental import pallas as pl
from jax.experimental.pallas import tpu as pltpu
from jax.sharding import PartitionSpec as P

RB = 8
LANES = 128
EDGE = 8
STRIDE = 32
CAPS = (21, 22, 23, 24, 25, 26, 28, 32)
C1, C2 = 8.0 / 12.0, 1.0 / 12.0
VMEM = pl.BlockSpec(memory_space=pltpu.VMEM)
SMEM = pl.BlockSpec(memory_space=pltpu.SMEM)


def lanes_of(rows):
    return lax.broadcasted_iota(jnp.int32, (rows, LANES), 1)


def params(mib):
    return pltpu.CompilerParams(vmem_limit_bytes=mib * 2**20)


def tiles_of(cap):
    return 2 * cap + -(-cap // 8)


def first(ahead, behind, ahead2, behind2):
    return C1 * (ahead - behind) - C2 * (ahead2 - behind2)


def second(centre, pairs):
    one, two, three, four = pairs
    return (four - 16.0 * three + 64.0 * two + 16.0 * one - 130.0 * centre) * (1.0 / 144.0)


def rows_of(window):
    def at(k):
        return window[8 + k : 24 + k, :]

    a1, b1, a2, b2 = at(1), at(-1), at(2), at(-2)
    slope = first(a1, b1, a2, b2)
    curve = second(at(0), (a1 + b1, a2 + b2, at(3) + at(-3), at(4) + at(-4)))
    return slope, curve


def slope_rows(window):
    def at(k):
        return window[8 + k : 24 + k, :]

    return first(at(1), at(-1), at(2), at(-2))


def shifted(field, beside, k, lane):
    if k > 0:
        return pltpu.roll(jnp.where(lane < k, beside, field), LANES - k, 1)
    return pltpu.roll(jnp.where(lane >= LANES + k, beside, field), -k, 1)


def columns_of(field, beside, lane):
    def at(k):
        return shifted(field, beside, k, lane)

    a1, b1, a2, b2 = at(1), at(-1), at(2), at(-2)
    slope_c = first(a1, b1, a2, b2)
    curve_cc = second(field, (a1 + b1, a2 + b2, at(3) + at(-3), at(4) + at(-4)))
    return slope_c, curve_cc


def column_slope(field, beside, lane):
    def at(k):
        return shifted(field, beside, k, lane)

    return first(at(1), at(-1), at(2), at(-2))


def near_kernel(blocks, p_ref, up_ref, down_ref, r_ref, c_ref, rr_ref, rc_ref, cc_ref, f_ref):
    lane = lanes_of(16)

    def rows(b, _):
        col = pl.multiple_of(b * LANES, LANES)
        base = pl.multiple_of(b * STRIDE, STRIDE)
        out = pl.multiple_of(b * 16, 16)
        window = f_ref.at[pl.ds(base, STRIDE), :]
        window[4:8, :] = up_ref[:, pl.ds(col, LANES)]
        window[8:24, :] = p_ref[:, pl.ds(col, LANES)]
        window[24:28, :] = down_ref[:, pl.ds(col, LANES)]
        slope, curve = rows_of(window)
        r_ref[pl.ds(out, 16), :] = slope
        rr_ref[pl.ds(out, 16), :] = curve
        return 0

    lax.fori_loop(0, blocks, rows, 0, unroll=8)

    def columns(b, _):
        before = lax.rem(b + (blocks - 1), blocks)
        after = lax.rem(b + 1, blocks)

        def of(i):
            return p_ref[:, pl.ds(pl.multiple_of(i * LANES, LANES), LANES)]

        def slope_of(i):
            return r_ref[pl.ds(pl.multiple_of(i * 16, 16), 16), :]

        far = lane >= LANES // 2
        slope_c, curve_cc = columns_of(of(b), jnp.where(far, of(before), of(after)), lane)
        curve_rc = column_slope(slope_of(b), jnp.where(far, slope_of(before), slope_of(after)), lane)
        out = pl.ds(pl.multiple_of(b * 16, 16), 16)
        c_ref[out, :] = slope_c
        rc_ref[out, :] = curve_rc
        cc_ref[out, :] = curve_cc
        return 0

    lax.fori_loop(0, blocks, columns, 0, unroll=8)


def near_fields(potentials, up, down):
    height, width = potentials.shape[1:]
    blocks = width // LANES
    shape = jax.ShapeDtypeStruct((blocks * 16, LANES), jnp.float32)
    return pl.pallas_call(
        functools.partial(near_kernel, blocks),
        grid=(1,),
        out_shape=(shape,) * 5,
        in_specs=[pl.BlockSpec((None, height, width), lambda i: (0, 0, 0)), VMEM, VMEM],
        out_specs=(VMEM,) * 5,
        scratch_shapes=[pltpu.VMEM((blocks * STRIDE, LANES), jnp.float32)],
        compiler_params=params(16),
        cost_estimate=pl.CostEstimate(flops=60_000_000, bytes_accessed=7_000_000, transcendentals=0),
        name="near_fields",
    )(potentials, up, down)


def index_kernel(blocks, caps, here_ref, row_ref, col_ref, table_ref, level_ref):
    lane = lax.broadcasted_iota(jnp.int32, (RB, blocks), 1)
    row = row_ref[...]
    alike = lax.broadcasted_iota(jnp.int32, (RB, blocks), 0) == row
    square = (blocks, blocks)
    upto = lax.broadcasted_iota(jnp.int32, square, 0) <= lax.broadcasted_iota(jnp.int32, square, 1)
    count = jnp.dot(alike.astype(jnp.float32), upto.astype(jnp.float32), preferred_element_type=jnp.float32)
    count = count.astype(jnp.int32)
    slot = jnp.sum(jnp.where(alike, count - 1, 0), axis=0, keepdims=True)
    source = lane[0:1] + col_ref[...]
    source = jnp.where(source >= blocks, source - blocks, source)
    needed = jnp.max(count)
    level = jnp.int32(0)
    tall, edges = jnp.int32(tiles_of(caps[0]) * 8), jnp.int32(16 * caps[0])
    for cap, following in zip(caps, caps[1:]):
        over = needed > cap
        level = level + over.astype(jnp.int32)
        tall = jnp.where(over, tiles_of(following) * 8, tall)
        edges = jnp.where(over, 16 * following, edges)
    level_ref[0] = level

    here = here_ref[0]
    edge_row = edges + (slot >> 3) * 8
    out_chunk = ((here + RB - row) & (RB - 1)) * tall
    in_chunk = ((here + row) & (RB - 1)) * tall
    turn = (lane[0:1] & 15) * EDGE + LANES - (slot & 7) * EDGE
    rows = (
        source * LANES,
        out_chunk + slot * 16,
        out_chunk + edge_row,
        slot & 7,
        in_chunk + slot * 16,
        in_chunk + edge_row,
        turn & (LANES - 1),
        (turn + LANES // 2) & (LANES - 1),
    )
    for k, values in enumerate(rows):
        table_ref[k : k + 1, :] = values


def index_of(row_offset, col_offset, here, caps):
    blocks = row_offset.shape[0]
    table, level = pl.pallas_call(
        functools.partial(index_kernel, blocks, caps),
        out_shape=(jax.ShapeDtypeStruct((8, blocks), jnp.int32), jax.ShapeDtypeStruct((1,), jnp.int32)),
        in_specs=[SMEM, VMEM, VMEM],
        out_specs=(VMEM, SMEM),
        name="block_index",
    )(here, row_offset.reshape(1, blocks), col_offset.reshape(1, blocks))
    return table, level[0]


def pack_kernel(blocks, cap, at_ref, p_in, out_hbm, p_ref, out_ref, in_sem, out_sem):
    width = blocks * LANES
    wide = width // 4
    loads = []
    for i in range(4):
        loads.append((pl.ds(i * wide, wide), pl.ds(LANES + i * wide, wide)))
    loads.append((pl.ds(width - LANES, LANES), pl.ds(0, LANES)))
    loads.append((pl.ds(0, LANES), pl.ds(width + LANES, LANES)))
    loads = [
        pltpu.make_async_copy(p_in.at[1, :, source], p_ref.at[:, target], in_sem.at[i])
        for i, (source, target) in enumerate(loads)
    ]
    for copy in loads:
        copy.start()
    lane = lanes_of(8)
    far = lane >= LANES // 2
    spots = lane // EDGE
    tall = tiles_of(cap) * 8
    for copy in loads:
        copy.wait()

    def block(b, _):
        col, row, edge_row, place = at_ref[0, b], at_ref[1, b], at_ref[2, b], at_ref[3, b]

        def of(i):
            return p_ref[:, pl.ds(pl.multiple_of(col + i * LANES, LANES), LANES)]

        out_ref[pl.ds(pl.multiple_of(row, 8), 16), :] = of(1)
        left, right = of(0), of(2)
        edge_rows = pl.ds(pl.multiple_of(edge_row, 8), 8)
        turn = place * EDGE + EDGE // 2
        for half in range(2):
            top = 8 * half
            edge = jnp.where(far, left[top : top + 8], right[top : top + 8])
            moved = pltpu.roll(edge, turn + half * (LANES // 2), 1)
            pltpu.store(out_ref.at[edge_rows, :], moved, mask=spots == place + 8 * half)
        return 0

    lax.fori_loop(0, blocks, block, 0, unroll=16)
    stores = []
    for i in range(RB):
        rows = pl.ds(i * tall, tall)
        stores.append(pltpu.make_async_copy(out_ref.at[rows, :], out_hbm.at[rows, :], out_sem.at[i]))
    for copy in stores:
        copy.start()
    for copy in stores:
        copy.wait()


def pack(cap, table, potentials):
    height, width = potentials.shape[1:]
    blocks = width // LANES
    shape = (RB * tiles_of(cap) * 8, LANES)
    return pl.pallas_call(
        functools.partial(pack_kernel, blocks, cap),
        out_shape=jax.ShapeDtypeStruct(shape, jnp.float32),
        in_specs=[SMEM, pl.BlockSpec(memory_space=pl.ANY)],
        out_specs=pl.BlockSpec(memory_space=pl.ANY),
        scratch_shapes=[
            pltpu.VMEM((height, width + 2 * LANES), jnp.float32),
            pltpu.VMEM(shape, jnp.float32),
            pltpu.SemaphoreType.DMA((6,)),
            pltpu.SemaphoreType.DMA((RB,)),
        ],
        compiler_params=params(24),
        cost_estimate=pl.CostEstimate(flops=2_000_000, bytes_accessed=3_000_000, transcendentals=0),
        name="pack_blocks",
    )(table, potentials)


def unpack_kernel(blocks, at_ref, in_ref, w_ref, h_ref, head_ref, tail_ref):
    spots = lanes_of(8) // EDGE

    def columns(group, _):
        edge_at = pl.multiple_of(group * 16, 16)
        for i in range(16):
            b = group * 16 + i
            row, edge_row, turn, half = at_ref[4, b], at_ref[5, b], at_ref[6, b], at_ref[7, b]
            tile = in_ref[pl.ds(pl.multiple_of(row, 8), 16), :]
            col = pl.ds(pl.multiple_of(b * LANES, LANES), LANES)
            w_ref[pl.ds(pl.multiple_of(b * 16, 16), 16), :] = tile
            head_ref[:, col] = tile[0:4]
            tail_ref[:, col] = tile[12:16]
            edge = in_ref[pl.ds(pl.multiple_of(edge_row, 8), 8), :]
            mask = spots == i
            pltpu.store(h_ref.at[pl.ds(edge_at, 8), :], pltpu.roll(edge, turn, 1), mask=mask)
            pltpu.store(h_ref.at[pl.ds(edge_at + 8, 8), :], pltpu.roll(edge, half, 1), mask=mask)
        return 0

    lax.fori_loop(0, blocks // 16, columns, 0)
    for g in range(blocks // 16):
        col = slice((blocks + g) * LANES, (blocks + g + 1) * LANES)
        head_ref[:, col] = h_ref[16 * g : 16 * g + 4, :]
        tail_ref[:, col] = h_ref[16 * g + 12 : 16 * g + 16, :]


def unpack(blocks, table, arrived):
    ends = jax.ShapeDtypeStruct((4, (blocks + blocks // 16) * LANES), jnp.float32)
    return pl.pallas_call(
        functools.partial(unpack_kernel, blocks),
        out_shape=(
            jax.ShapeDtypeStruct((blocks * 16, LANES), jnp.float32),
            jax.ShapeDtypeStruct((blocks, LANES), jnp.float32),
            ends,
            ends,
        ),
        in_specs=[SMEM, VMEM],
        out_specs=(VMEM,) * 4,
        compiler_params=params(24),
        cost_estimate=pl.CostEstimate(flops=2_000_000, bytes_accessed=3_000_000, transcendentals=0),
        name="unpack_blocks",
    )(table, arrived)


def edge_turn(b):
    return LANES - EDGE // 2 - b * EDGE


def columns_kernel(blocks, h_ref, w_in, n0, n1, n2, n3, n4, c_ref, cc_ref, w_ref, m0, m1, m2, m3, m4, g_ref, w_sem, sem):
    lane = lanes_of(16)
    quarter = blocks * 4

    def part(i):
        rows = pl.ds(i * quarter, quarter)
        return pltpu.make_async_copy(w_in.at[rows, :], w_ref.at[rows, :], w_sem.at[i])

    near = [pltpu.make_async_copy(n, m, sem.at[i]) for i, (n, m) in enumerate(zip((n0, n1, n2, n3, n4), (m0, m1, m2, m3, m4)))]
    for i in range(4):
        part(i).start()

    def spread(i, _):
        edge = h_ref[pl.ds(pl.multiple_of(i * 16, 16), 16), :]
        for k in range(16):
            g_ref[pl.ds(pl.multiple_of(i * 256 + k * 16, 16), 16), :] = pltpu.roll(edge, edge_turn(k), 1)
        return 0

    lax.fori_loop(0, blocks // 16, spread, 0)
    for i in range(4):
        part(i).wait()
    for copy in near:
        copy.start()

    def block(b, _):
        tile = pl.ds(pl.multiple_of(b * 16, 16), 16)
        c_ref[tile, :], cc_ref[tile, :] = columns_of(w_ref[tile, :], g_ref[tile, :], lane)
        return 0

    lax.fori_loop(0, blocks, block, 0, unroll=8)
    for copy in near:
        copy.wait()


def far_columns(windows, edges, near):
    blocks = edges.shape[0]
    anywhere = pl.BlockSpec(memory_space=pl.ANY)
    out = pl.pallas_call(
        functools.partial(columns_kernel, blocks),
        out_shape=(jax.ShapeDtypeStruct(windows.shape, jnp.float32),) * 8,
        in_specs=[VMEM] + [anywhere] * 6,
        out_specs=(VMEM,) * 8,
        scratch_shapes=[
            pltpu.VMEM(windows.shape, jnp.float32),
            pltpu.SemaphoreType.DMA((4,)),
            pltpu.SemaphoreType.DMA((5,)),
        ],
        compiler_params=params(16),
        cost_estimate=pl.CostEstimate(flops=20_000_000, bytes_accessed=3_000_000, transcendentals=0),
        name="far_columns",
    )(edges, windows, *near)
    return out[:2], out[2], out[3:]


def far_kernel(
    ratio_ref, w_ref, h_ref, up_ref, down_ref, far_c_ref, far_cc_ref, r_ref, c_ref, rr_ref, rc_ref, cc_ref,
    conv_out, shear_out, rot_out, disp_out, conv_ref, shear_ref, rot_ref, disp_ref, f_ref, e_ref, s_ref, sem,
):
    blocks = h_ref.shape[0]
    lane = lanes_of(16)
    near_to_two, near_to_source, two_to_source = ratio_ref[0], ratio_ref[1], ratio_ref[2]
    half_one, half_two = 0.5 * near_to_source, 0.5 * two_to_source
    refs = ((conv_ref, conv_out), (shear_ref, shear_out), (rot_ref, rot_out), (disp_ref, disp_out))

    def copies(group):
        cols = pl.ds(pl.multiple_of(group * 16 * LANES, 16 * LANES), 16 * LANES)
        return [
            pltpu.make_async_copy(ref.at[..., cols], out.at[..., cols], sem.at[k, group]) for k, (ref, out) in enumerate(refs)
        ]

    def columns(group, _):
        ends = pl.ds(pl.multiple_of((blocks + group) * LANES, LANES), LANES)
        e_ref[4:8, :] = up_ref[:, ends]
        e_ref[8:24, :] = h_ref[pl.ds(pl.multiple_of(group * 16, 16), 16), :]
        e_ref[24:28, :] = down_ref[:, ends]
        s_ref[...] = slope_rows(e_ref)

        def block(i, _):
            b = group * 16 + i
            col = pl.ds(pl.multiple_of(b * LANES, LANES), LANES)
            tile = pl.ds(pl.multiple_of(b * 16, 16), 16)
            window = f_ref.at[pl.ds(pl.multiple_of(i * STRIDE, STRIDE), STRIDE), :]
            window[4:8, :] = up_ref[:, col]
            window[8:24, :] = w_ref[tile, :]
            window[24:28, :] = down_ref[:, col]
            far_r, far_rr = rows_of(window)
            far_rc = column_slope(far_r, pltpu.roll(s_ref[...], edge_turn(i), 1), lane)
            far_cc = far_cc_ref[tile, :]
            near_rr, near_rc, near_cc = rr_ref[tile, :], rc_ref[tile, :], cc_ref[tile, :]
            inner_rr = 1.0 - near_to_two * near_rr
            inner_rc = -near_to_two * near_rc
            inner_cc = 1.0 - near_to_two * near_cc
            chain_rr = far_rr * inner_rr + far_rc * inner_rc
            chain_rc = far_rr * inner_rc + far_rc * inner_cc
            chain_cr = far_rc * inner_rr + far_cc * inner_rc
            chain_cc = far_rc * inner_rc + far_cc * inner_cc
            conv_ref[:, col] = half_one * (near_rr + near_cc) + half_two * (chain_rr + chain_cc)
            shear_ref[0, :, col] = half_one * (near_cc - near_rr) + half_two * (chain_cc - chain_rr)
            shear_ref[1, :, col] = near_to_source * near_rc + half_two * (chain_rc + chain_cr)
            rot_ref[:, col] = half_two * (chain_cr - chain_rc)
            disp_ref[0, :, col] = near_to_source * r_ref[tile, :] + two_to_source * far_r
            disp_ref[1, :, col] = near_to_source * c_ref[tile, :] + two_to_source * far_c_ref[tile, :]
            return 0

        lax.fori_loop(0, 16, block, 0, unroll=16)
        for copy in copies(group):
            copy.start()
        return 0

    lax.fori_loop(0, blocks // 16, columns, 0)

    def finish(group, _):
        for copy in copies(group):
            copy.wait()
        return 0

    lax.fori_loop(0, blocks // 16, finish, 0)


def assemble(ratios, windows, edges, above, below, far, near):
    blocks = edges.shape[0]
    flat = jax.ShapeDtypeStruct((16, blocks * LANES), jnp.float32)
    pair = jax.ShapeDtypeStruct((2, 16, blocks * LANES), jnp.float32)
    outs = (flat, pair, flat, pair)
    return pl.pallas_call(
        far_kernel,
        out_shape=outs,
        in_specs=[SMEM] + [VMEM] * 11,
        out_specs=(pl.BlockSpec(memory_space=pl.ANY),) * 4,
        scratch_shapes=[pltpu.VMEM(o.shape, o.dtype) for o in outs]
        + [
            pltpu.VMEM((16 * STRIDE, LANES), jnp.float32),
            pltpu.VMEM((STRIDE, LANES), jnp.float32),
            pltpu.VMEM((16, LANES), jnp.float32),
            pltpu.SemaphoreType.DMA((4, blocks // 16)),
        ],
        compiler_params=params(16),
        cost_estimate=pl.CostEstimate(flops=40_000_000, bytes_accessed=6_000_000, transcendentals=0),
        name="far_fields",
    )(ratios, windows, edges, above, below, *far, *near)


def passed(x, by):
    size = lax.axis_size("row")
    return lax.ppermute(x, "row", [(i, (i + by) % size) for i in range(size)])


def near_plane(potentials):
    height = potentials.shape[1]
    above = passed(potentials[0, height - 4 :, :], 1)
    below = passed(potentials[0, :4, :], -1)
    return near_fields(potentials, above, below)


def near_blank(potentials):
    width = potentials.shape[2]
    return (jnp.zeros((width // LANES * 16, LANES), jnp.float32),) * 5


def exchange(cap, groups, potentials, here, table):
    blocks = potentials.shape[2] // LANES
    packed = pack(cap, table, potentials)
    packed = packed.reshape(RB, tiles_of(cap) * 8, LANES)
    arrived = lax.all_to_all(packed, "row", 0, 0, axis_index_groups=groups)
    near = lax.cond(here[0] >= 0, near_plane, near_blank, potentials)
    arrived = arrived.reshape(RB * tiles_of(cap) * 8, LANES)
    return unpack(blocks, table, arrived), near


def per_device(potentials, ratios, row_offset, col_offset):
    stride = lax.axis_size("row") // RB
    blocks = potentials.shape[2] // LANES
    caps = tuple(c for c in CAPS if c < blocks) + (blocks,)
    here = (lax.axis_index("row") // stride).astype(jnp.int32).reshape(1)
    table, level = index_of(row_offset, col_offset, here, caps)
    groups = [[y * stride + j for y in range(RB)] for j in range(stride)]
    (windows, edges, heads, tails), near = lax.switch(
        level,
        [functools.partial(exchange, cap, groups) for cap in caps],
        potentials, here, table,
    )
    above = passed(tails, 1)
    below = passed(heads, -1)
    far, windows, near = far_columns(windows, edges, near)
    return assemble(ratios, windows, edges, above, below, far, near)


def solution(mesh):
    return jax.shard_map(
        per_device,
        mesh=mesh,
        in_specs=(P("cosmo", "row", None), P("cosmo"), P("cosmo"), P("cosmo")),
        out_specs=(
            P(("cosmo", "row"), None),
            P(None, ("cosmo", "row"), None),
            P(("cosmo", "row"), None),
            P(None, ("cosmo", "row"), None),
        ),
        check_vma=False,
    )
```

```python
import functools

import jax
import jax.numpy as jnp
from jax import lax
from jax.experimental import pallas as pl
from jax.experimental.pallas import tpu as pltpu
from jax.sharding import PartitionSpec as P

RB = 8
LANES = 128
EDGE = 8
STRIDE = 32
CAPS = (21, 22, 23, 24, 25, 26, 28, 32)
C1, C2 = 8.0 / 12.0, 1.0 / 12.0
VMEM = pl.BlockSpec(memory_space=pltpu.VMEM)
SMEM = pl.BlockSpec(memory_space=pltpu.SMEM)


def lanes_of(rows):
    return lax.broadcasted_iota(jnp.int32, (rows, LANES), 1)


def params(mib):
    return pltpu.CompilerParams(vmem_limit_bytes=mib * 2**20)


def tiles_of(cap):
    return 2 * cap + -(-cap // 8)


def first(ahead, behind, ahead2, behind2):
    return C1 * (ahead - behind) - C2 * (ahead2 - behind2)


def second(centre, pairs):
    one, two, three, four = pairs
    return (1.0 / 9.0) * (one - three) + (4.0 / 9.0) * two + (1.0 / 144.0) * four - (130.0 / 144.0) * centre


def rows_of(window):
    def at(k):
        return window[8 + k : 24 + k, :]

    a1, b1, a2, b2 = at(1), at(-1), at(2), at(-2)
    slope = first(a1, b1, a2, b2)
    curve = second(at(0), (a1 + b1, a2 + b2, at(3) + at(-3), at(4) + at(-4)))
    return slope, curve


def slope_rows(window):
    def at(k):
        return window[8 + k : 24 + k, :]

    return first(at(1), at(-1), at(2), at(-2))


def shifted(field, beside, k, lane):
    if k > 0:
        return pltpu.roll(jnp.where(lane < k, beside, field), LANES - k, 1)
    return pltpu.roll(jnp.where(lane >= LANES + k, beside, field), -k, 1)


def columns_of(field, beside, lane):
    def at(k):
        return shifted(field, beside, k, lane)

    a1, b1, a2, b2 = at(1), at(-1), at(2), at(-2)
    slope_c = first(a1, b1, a2, b2)
    curve_cc = second(field, (a1 + b1, a2 + b2, at(3) + at(-3), at(4) + at(-4)))
    return slope_c, curve_cc


def column_slope(field, beside, lane):
    def at(k):
        return shifted(field, beside, k, lane)

    return first(at(1), at(-1), at(2), at(-2))


def near_kernel(blocks, p_ref, up_ref, down_ref, r_ref, c_ref, rr_ref, rc_ref, cc_ref, f_ref):
    lane = lanes_of(16)

    def rows(b, _):
        col = pl.multiple_of(b * LANES, LANES)
        base = pl.multiple_of(b * STRIDE, STRIDE)
        out = pl.multiple_of(b * 16, 16)
        window = f_ref.at[pl.ds(base, STRIDE), :]
        window[4:8, :] = up_ref[:, pl.ds(col, LANES)]
        window[8:24, :] = p_ref[:, pl.ds(col, LANES)]
        window[24:28, :] = down_ref[:, pl.ds(col, LANES)]
        slope, curve = rows_of(window)
        r_ref[pl.ds(out, 16), :] = slope
        rr_ref[pl.ds(out, 16), :] = curve
        return 0

    lax.fori_loop(0, blocks, rows, 0, unroll=8)

    def columns(b, _):
        before = lax.rem(b + (blocks - 1), blocks)
        after = lax.rem(b + 1, blocks)

        def of(i):
            return p_ref[:, pl.ds(pl.multiple_of(i * LANES, LANES), LANES)]

        def slope_of(i):
            return r_ref[pl.ds(pl.multiple_of(i * 16, 16), 16), :]

        far = lane >= LANES // 2
        slope_c, curve_cc = columns_of(of(b), jnp.where(far, of(before), of(after)), lane)
        curve_rc = column_slope(slope_of(b), jnp.where(far, slope_of(before), slope_of(after)), lane)
        out = pl.ds(pl.multiple_of(b * 16, 16), 16)
        c_ref[out, :] = slope_c
        rc_ref[out, :] = curve_rc
        cc_ref[out, :] = curve_cc
        return 0

    lax.fori_loop(0, blocks, columns, 0, unroll=8)


def near_fields(potentials, up, down):
    height, width = potentials.shape[1:]
    blocks = width // LANES
    shape = jax.ShapeDtypeStruct((blocks * 16, LANES), jnp.float32)
    return pl.pallas_call(
        functools.partial(near_kernel, blocks),
        grid=(1,),
        out_shape=(shape,) * 5,
        in_specs=[pl.BlockSpec((None, height, width), lambda i: (0, 0, 0)), VMEM, VMEM],
        out_specs=(VMEM,) * 5,
        scratch_shapes=[pltpu.VMEM((blocks * STRIDE, LANES), jnp.float32)],
        compiler_params=params(16),
        cost_estimate=pl.CostEstimate(flops=60_000_000, bytes_accessed=7_000_000, transcendentals=0),
        name="near_fields",
    )(potentials, up, down)


def index_kernel(blocks, caps, here_ref, row_ref, col_ref, table_ref, level_ref):
    lane = lax.broadcasted_iota(jnp.int32, (RB, blocks), 1)
    row = row_ref[...]
    alike = lax.broadcasted_iota(jnp.int32, (RB, blocks), 0) == row
    square = (blocks, blocks)
    upto = lax.broadcasted_iota(jnp.int32, square, 0) <= lax.broadcasted_iota(jnp.int32, square, 1)
    count = jnp.dot(alike.astype(jnp.float32), upto.astype(jnp.float32), preferred_element_type=jnp.float32)
    count = count.astype(jnp.int32)
    slot = jnp.sum(jnp.where(alike, count - 1, 0), axis=0, keepdims=True)
    source = lane[0:1] + col_ref[...]
    source = jnp.where(source >= blocks, source - blocks, source)
    needed = jnp.max(count)
    level = jnp.int32(0)
    tall, edges = jnp.int32(tiles_of(caps[0]) * 8), jnp.int32(16 * caps[0])
    for cap, following in zip(caps, caps[1:]):
        over = needed > cap
        level = level + over.astype(jnp.int32)
        tall = jnp.where(over, tiles_of(following) * 8, tall)
        edges = jnp.where(over, 16 * following, edges)
    level_ref[0] = level

    here = here_ref[0]
    edge_row = edges + (slot >> 3) * 8
    out_chunk = ((here + RB - row) & (RB - 1)) * tall
    in_chunk = ((here + row) & (RB - 1)) * tall
    turn = (lane[0:1] & 15) * EDGE + LANES - (slot & 7) * EDGE
    rows = (
        source * LANES,
        out_chunk + slot * 16,
        out_chunk + edge_row,
        slot & 7,
        in_chunk + slot * 16,
        in_chunk + edge_row,
        turn & (LANES - 1),
        (turn + LANES // 2) & (LANES - 1),
    )
    for k, values in enumerate(rows):
        table_ref[k : k + 1, :] = values


def index_of(row_offset, col_offset, here, caps):
    blocks = row_offset.shape[0]
    table, level = pl.pallas_call(
        functools.partial(index_kernel, blocks, caps),
        out_shape=(jax.ShapeDtypeStruct((8, blocks), jnp.int32), jax.ShapeDtypeStruct((1,), jnp.int32)),
        in_specs=[SMEM, VMEM, VMEM],
        out_specs=(VMEM, SMEM),
        name="block_index",
    )(here, row_offset.reshape(1, blocks), col_offset.reshape(1, blocks))
    return table, level[0]


def pack_kernel(blocks, cap, at_ref, p_in, out_hbm, p_ref, out_ref, in_sem, out_sem):
    width = blocks * LANES
    wide = width // 4
    loads = []
    for i in range(4):
        loads.append((pl.ds(i * wide, wide), pl.ds(LANES + i * wide, wide)))
    loads.append((pl.ds(width - LANES, LANES), pl.ds(0, LANES)))
    loads.append((pl.ds(0, LANES), pl.ds(width + LANES, LANES)))
    loads = [
        pltpu.make_async_copy(p_in.at[1, :, source], p_ref.at[:, target], in_sem.at[i])
        for i, (source, target) in enumerate(loads)
    ]
    for copy in loads:
        copy.start()
    lane = lanes_of(8)
    far = lane >= LANES // 2
    spots = lane // EDGE
    tall = tiles_of(cap) * 8
    for copy in loads:
        copy.wait()

    def block(b, _):
        col, row, edge_row, place = at_ref[0, b], at_ref[1, b], at_ref[2, b], at_ref[3, b]

        def of(i):
            return p_ref[:, pl.ds(pl.multiple_of(col + i * LANES, LANES), LANES)]

        out_ref[pl.ds(pl.multiple_of(row, 8), 16), :] = of(1)
        left, right = of(0), of(2)
        edge_rows = pl.ds(pl.multiple_of(edge_row, 8), 8)
        turn = place * EDGE + EDGE // 2
        for half in range(2):
            top = 8 * half
            edge = jnp.where(far, left[top : top + 8], right[top : top + 8])
            moved = pltpu.roll(edge, turn + half * (LANES // 2), 1)
            pltpu.store(out_ref.at[edge_rows, :], moved, mask=spots == place + 8 * half)
        return 0

    lax.fori_loop(0, blocks, block, 0, unroll=16)
    stores = []
    for i in range(RB):
        rows = pl.ds(i * tall, tall)
        stores.append(pltpu.make_async_copy(out_ref.at[rows, :], out_hbm.at[rows, :], out_sem.at[i]))
    for copy in stores:
        copy.start()
    for copy in stores:
        copy.wait()


def pack(cap, table, potentials):
    height, width = potentials.shape[1:]
    blocks = width // LANES
    shape = (RB * tiles_of(cap) * 8, LANES)
    return pl.pallas_call(
        functools.partial(pack_kernel, blocks, cap),
        out_shape=jax.ShapeDtypeStruct(shape, jnp.float32),
        in_specs=[SMEM, pl.BlockSpec(memory_space=pl.ANY)],
        out_specs=pl.BlockSpec(memory_space=pl.ANY),
        scratch_shapes=[
            pltpu.VMEM((height, width + 2 * LANES), jnp.float32),
            pltpu.VMEM(shape, jnp.float32),
            pltpu.SemaphoreType.DMA((6,)),
            pltpu.SemaphoreType.DMA((RB,)),
        ],
        compiler_params=params(24),
        cost_estimate=pl.CostEstimate(flops=2_000_000, bytes_accessed=3_000_000, transcendentals=0),
        name="pack_blocks",
    )(table, potentials)


def unpack_kernel(blocks, at_ref, in_ref, w_ref, h_ref, head_ref, tail_ref):
    spots = lanes_of(8) // EDGE

    def columns(group, _):
        edge_at = pl.multiple_of(group * 16, 16)
        for i in range(16):
            b = group * 16 + i
            row, edge_row, turn, half = at_ref[4, b], at_ref[5, b], at_ref[6, b], at_ref[7, b]
            tile = in_ref[pl.ds(pl.multiple_of(row, 8), 16), :]
            col = pl.ds(pl.multiple_of(b * LANES, LANES), LANES)
            w_ref[pl.ds(pl.multiple_of(b * 16, 16), 16), :] = tile
            head_ref[:, col] = tile[0:4]
            tail_ref[:, col] = tile[12:16]
            edge = in_ref[pl.ds(pl.multiple_of(edge_row, 8), 8), :]
            mask = spots == i
            pltpu.store(h_ref.at[pl.ds(edge_at, 8), :], pltpu.roll(edge, turn, 1), mask=mask)
            pltpu.store(h_ref.at[pl.ds(edge_at + 8, 8), :], pltpu.roll(edge, half, 1), mask=mask)
        return 0

    lax.fori_loop(0, blocks // 16, columns, 0)
    for g in range(blocks // 16):
        col = slice((blocks + g) * LANES, (blocks + g + 1) * LANES)
        head_ref[:, col] = h_ref[16 * g : 16 * g + 4, :]
        tail_ref[:, col] = h_ref[16 * g + 12 : 16 * g + 16, :]


def unpack(blocks, table, arrived):
    ends = jax.ShapeDtypeStruct((4, (blocks + blocks // 16) * LANES), jnp.float32)
    return pl.pallas_call(
        functools.partial(unpack_kernel, blocks),
        out_shape=(
            jax.ShapeDtypeStruct((blocks * 16, LANES), jnp.float32),
            jax.ShapeDtypeStruct((blocks, LANES), jnp.float32),
            ends,
            ends,
        ),
        in_specs=[SMEM, VMEM],
        out_specs=(VMEM,) * 4,
        compiler_params=params(24),
        cost_estimate=pl.CostEstimate(flops=2_000_000, bytes_accessed=3_000_000, transcendentals=0),
        name="unpack_blocks",
    )(table, arrived)


def edge_turn(b):
    return LANES - EDGE // 2 - b * EDGE


def columns_kernel(blocks, h_ref, w_ref, n0, n1, n2, n3, n4, c_ref, cc_ref, m0, m1, m2, m3, m4, g_ref, sem):
    lane = lanes_of(16)
    near = [pltpu.make_async_copy(n, m, sem.at[i]) for i, (n, m) in enumerate(zip((n0, n1, n2, n3, n4), (m0, m1, m2, m3, m4)))]
    for copy in near:
        copy.start()

    def spread(i, _):
        edge = h_ref[pl.ds(pl.multiple_of(i * 16, 16), 16), :]
        for k in range(16):
            g_ref[pl.ds(pl.multiple_of(i * 256 + k * 16, 16), 16), :] = pltpu.roll(edge, edge_turn(k), 1)
        return 0

    lax.fori_loop(0, blocks // 16, spread, 0, unroll=4)

    def block(b, _):
        tile = pl.ds(pl.multiple_of(b * 16, 16), 16)
        c_ref[tile, :], cc_ref[tile, :] = columns_of(w_ref[tile, :], g_ref[tile, :], lane)
        return 0

    lax.fori_loop(0, blocks, block, 0, unroll=16)
    for copy in near:
        copy.wait()


def far_columns(windows, edges, near):
    blocks = edges.shape[0]
    anywhere = pl.BlockSpec(memory_space=pl.ANY)
    out = pl.pallas_call(
        functools.partial(columns_kernel, blocks),
        out_shape=(jax.ShapeDtypeStruct(windows.shape, jnp.float32),) * 7,
        in_specs=[VMEM] * 2 + [anywhere] * 5,
        out_specs=(VMEM,) * 7,
        scratch_shapes=[
            pltpu.VMEM(windows.shape, jnp.float32),
            pltpu.SemaphoreType.DMA((5,)),
        ],
        compiler_params=params(16),
        cost_estimate=pl.CostEstimate(flops=20_000_000, bytes_accessed=3_000_000, transcendentals=0),
        name="far_columns",
    )(edges, windows, *near)
    return out[:2], out[2:]


def far_kernel(
    ratio_ref, w_ref, h_ref, up_ref, down_ref, far_c_ref, far_cc_ref, r_ref, c_ref, rr_ref, rc_ref, cc_ref,
    conv_out, shear_out, rot_out, disp_out, conv_ref, shear_ref, rot_ref, disp_ref, f_ref, e_ref, s_ref, sem,
):
    blocks = h_ref.shape[0]
    lane = lanes_of(16)
    near_to_two, near_to_source, two_to_source = ratio_ref[0], ratio_ref[1], ratio_ref[2]
    half_one, half_two = 0.5 * near_to_source, 0.5 * two_to_source
    half_near = half_two * near_to_two
    refs = ((conv_ref, conv_out), (shear_ref, shear_out), (rot_ref, rot_out), (disp_ref, disp_out))

    def copies(group):
        cols = pl.ds(pl.multiple_of(group * 16 * LANES, 16 * LANES), 16 * LANES)
        return [
            pltpu.make_async_copy(ref.at[..., cols], out.at[..., cols], sem.at[k, group]) for k, (ref, out) in enumerate(refs)
        ]

    def columns(group, _):
        ends = pl.ds(pl.multiple_of((blocks + group) * LANES, LANES), LANES)
        e_ref[4:8, :] = up_ref[:, ends]
        e_ref[8:24, :] = h_ref[pl.ds(pl.multiple_of(group * 16, 16), 16), :]
        e_ref[24:28, :] = down_ref[:, ends]
        s_ref[...] = slope_rows(e_ref)

        def block(i, _):
            b = group * 16 + i
            col = pl.ds(pl.multiple_of(b * LANES, LANES), LANES)
            tile = pl.ds(pl.multiple_of(b * 16, 16), 16)
            window = f_ref.at[pl.ds(pl.multiple_of(i * STRIDE, STRIDE), STRIDE), :]
            window[4:8, :] = up_ref[:, col]
            window[8:24, :] = w_ref[tile, :]
            window[24:28, :] = down_ref[:, col]
            far_r, far_rr = rows_of(window)
            far_rc = column_slope(far_r, pltpu.roll(s_ref[...], edge_turn(i), 1), lane)
            far_cc = far_cc_ref[tile, :]
            near_rr, near_rc, near_cc = rr_ref[tile, :], rc_ref[tile, :], cc_ref[tile, :]
            inner_rr = half_two - half_near * near_rr
            inner_rc = -half_near * near_rc
            inner_cc = half_two - half_near * near_cc
            chain_rr = far_rr * inner_rr + far_rc * inner_rc
            chain_rc = far_rr * inner_rc + far_rc * inner_cc
            chain_cr = far_rc * inner_rr + far_cc * inner_rc
            chain_cc = far_rc * inner_rc + far_cc * inner_cc
            conv_ref[:, col] = half_one * (near_rr + near_cc) + (chain_rr + chain_cc)
            shear_ref[0, :, col] = half_one * (near_cc - near_rr) + (chain_cc - chain_rr)
            shear_ref[1, :, col] = near_to_source * near_rc + (chain_rc + chain_cr)
            rot_ref[:, col] = chain_cr - chain_rc
            disp_ref[0, :, col] = near_to_source * r_ref[tile, :] + two_to_source * far_r
            disp_ref[1, :, col] = near_to_source * c_ref[tile, :] + two_to_source * far_c_ref[tile, :]
            return 0

        lax.fori_loop(0, 16, block, 0, unroll=16)
        for copy in copies(group):
            copy.start()
        return 0

    lax.fori_loop(0, blocks // 16, columns, 0)

    def finish(group, _):
        for copy in copies(group):
            copy.wait()
        return 0

    lax.fori_loop(0, blocks // 16, finish, 0)


def assemble(ratios, windows, edges, above, below, far, near):
    blocks = edges.shape[0]
    flat = jax.ShapeDtypeStruct((16, blocks * LANES), jnp.float32)
    pair = jax.ShapeDtypeStruct((2, 16, blocks * LANES), jnp.float32)
    outs = (flat, pair, flat, pair)
    return pl.pallas_call(
        far_kernel,
        out_shape=outs,
        in_specs=[SMEM] + [VMEM] * 11,
        out_specs=(pl.BlockSpec(memory_space=pl.ANY),) * 4,
        scratch_shapes=[pltpu.VMEM(o.shape, o.dtype) for o in outs]
        + [
            pltpu.VMEM((16 * STRIDE, LANES), jnp.float32),
            pltpu.VMEM((STRIDE, LANES), jnp.float32),
            pltpu.VMEM((16, LANES), jnp.float32),
            pltpu.SemaphoreType.DMA((4, blocks // 16)),
        ],
        compiler_params=params(16),
        cost_estimate=pl.CostEstimate(flops=40_000_000, bytes_accessed=6_000_000, transcendentals=0),
        name="far_fields",
    )(ratios, windows, edges, above, below, *far, *near)


def passed(x, by):
    size = lax.axis_size("row")
    return lax.ppermute(x, "row", [(i, (i + by) % size) for i in range(size)])


def near_plane(potentials):
    height = potentials.shape[1]
    above = passed(potentials[0, height - 4 :, :], 1)
    below = passed(potentials[0, :4, :], -1)
    return near_fields(potentials, above, below)


def near_blank(potentials):
    width = potentials.shape[2]
    return (jnp.zeros((width // LANES * 16, LANES), jnp.float32),) * 5


def exchange(cap, groups, potentials, here, table):
    blocks = potentials.shape[2] // LANES
    packed = pack(cap, table, potentials)
    packed = packed.reshape(RB, tiles_of(cap) * 8, LANES)
    arrived = lax.all_to_all(packed, "row", 0, 0, axis_index_groups=groups)
    near = lax.cond(here[0] >= 0, near_plane, near_blank, potentials)
    arrived = arrived.reshape(RB * tiles_of(cap) * 8, LANES)
    return unpack(blocks, table, arrived), near


def per_device(potentials, ratios, row_offset, col_offset):
    stride = lax.axis_size("row") // RB
    blocks = potentials.shape[2] // LANES
    caps = tuple(c for c in CAPS if c < blocks) + (blocks,)
    here = (lax.axis_index("row") // stride).astype(jnp.int32).reshape(1)
    table, level = index_of(row_offset, col_offset, here, caps)
    groups = [[y * stride + j for y in range(RB)] for j in range(stride)]
    (windows, edges, heads, tails), near = lax.switch(
        level,
        [functools.partial(exchange, cap, groups) for cap in caps],
        potentials, here, table,
    )
    above = passed(tails, 1)
    below = passed(heads, -1)
    far, near = far_columns(windows, edges, near)
    return assemble(ratios, windows, edges, above, below, far, near)


def solution(mesh):
    return jax.shard_map(
        per_device,
        mesh=mesh,
        in_specs=(P("cosmo", "row", None), P("cosmo"), P("cosmo"), P("cosmo")),
        out_specs=(
            P(("cosmo", "row"), None),
            P(None, ("cosmo", "row"), None),
            P(("cosmo", "row"), None),
            P(None, ("cosmo", "row"), None),
        ),
        check_vma=False,
    )
```

```python
import functools

import jax
import jax.numpy as jnp
from jax import lax
from jax.experimental import pallas as pl
from jax.experimental.pallas import tpu as pltpu
from jax.sharding import PartitionSpec as P

RB = 8
LANES = 128
EDGE = 8
STRIDE = 32
CAPS = (21, 22, 23, 24, 25, 26, 28, 32)
C1, C2 = 8.0 / 12.0, 1.0 / 12.0
VMEM = pl.BlockSpec(memory_space=pltpu.VMEM)
SMEM = pl.BlockSpec(memory_space=pltpu.SMEM)


def lanes_of(rows):
    return lax.broadcasted_iota(jnp.int32, (rows, LANES), 1)


def params(mib):
    return pltpu.CompilerParams(vmem_limit_bytes=mib * 2**20)


def tiles_of(cap):
    return 2 * cap + -(-cap // 8)


def first(ahead, behind, ahead2, behind2):
    return C1 * (ahead - behind) - C2 * (ahead2 - behind2)


def second(centre, pairs):
    one, two, three, four = pairs
    return (four - 16.0 * three + 64.0 * two + 16.0 * one - 130.0 * centre) * (1.0 / 144.0)


def rows_of(window):
    def at(k):
        return window[8 + k : 24 + k, :]

    a1, b1, a2, b2 = at(1), at(-1), at(2), at(-2)
    slope = first(a1, b1, a2, b2)
    curve = second(at(0), (a1 + b1, a2 + b2, at(3) + at(-3), at(4) + at(-4)))
    return slope, curve


def slope_rows(window):
    def at(k):
        return window[8 + k : 24 + k, :]

    return first(at(1), at(-1), at(2), at(-2))


def shifted(field, beside, k, lane):
    if k > 0:
        return pltpu.roll(jnp.where(lane < k, beside, field), LANES - k, 1)
    return pltpu.roll(jnp.where(lane >= LANES + k, beside, field), -k, 1)


def columns_of(field, beside, lane):
    def at(k):
        return shifted(field, beside, k, lane)

    a1, b1, a2, b2 = at(1), at(-1), at(2), at(-2)
    slope_c = first(a1, b1, a2, b2)
    curve_cc = second(field, (a1 + b1, a2 + b2, at(3) + at(-3), at(4) + at(-4)))
    return slope_c, curve_cc


def column_slope(field, beside, lane):
    def at(k):
        return shifted(field, beside, k, lane)

    return first(at(1), at(-1), at(2), at(-2))


def near_kernel(blocks, p_ref, up_ref, down_ref, r_ref, c_ref, rr_ref, rc_ref, cc_ref, f_ref):
    lane = lanes_of(16)

    def rows(b, _):
        col = pl.multiple_of(b * LANES, LANES)
        base = pl.multiple_of(b * STRIDE, STRIDE)
        out = pl.multiple_of(b * 16, 16)
        window = f_ref.at[pl.ds(base, STRIDE), :]
        window[4:8, :] = up_ref[:, pl.ds(col, LANES)]
        window[8:24, :] = p_ref[:, pl.ds(col, LANES)]
        window[24:28, :] = down_ref[:, pl.ds(col, LANES)]
        slope, curve = rows_of(window)
        r_ref[pl.ds(out, 16), :] = slope
        rr_ref[pl.ds(out, 16), :] = curve
        return 0

    lax.fori_loop(0, blocks, rows, 0, unroll=8)

    def columns(b, _):
        before = lax.rem(b + (blocks - 1), blocks)
        after = lax.rem(b + 1, blocks)

        def of(i):
            return p_ref[:, pl.ds(pl.multiple_of(i * LANES, LANES), LANES)]

        def slope_of(i):
            return r_ref[pl.ds(pl.multiple_of(i * 16, 16), 16), :]

        far = lane >= LANES // 2
        slope_c, curve_cc = columns_of(of(b), jnp.where(far, of(before), of(after)), lane)
        curve_rc = column_slope(slope_of(b), jnp.where(far, slope_of(before), slope_of(after)), lane)
        out = pl.ds(pl.multiple_of(b * 16, 16), 16)
        c_ref[out, :] = slope_c
        rc_ref[out, :] = curve_rc
        cc_ref[out, :] = curve_cc
        return 0

    lax.fori_loop(0, blocks, columns, 0, unroll=8)


def near_fields(potentials, up, down):
    height, width = potentials.shape[1:]
    blocks = width // LANES
    shape = jax.ShapeDtypeStruct((blocks * 16, LANES), jnp.float32)
    return pl.pallas_call(
        functools.partial(near_kernel, blocks),
        grid=(1,),
        out_shape=(shape,) * 5,
        in_specs=[pl.BlockSpec((None, height, width), lambda i: (0, 0, 0)), VMEM, VMEM],
        out_specs=(VMEM,) * 5,
        scratch_shapes=[pltpu.VMEM((blocks * STRIDE, LANES), jnp.float32)],
        compiler_params=params(16),
        cost_estimate=pl.CostEstimate(flops=60_000_000, bytes_accessed=7_000_000, transcendentals=0),
        name="near_fields",
    )(potentials, up, down)


def index_kernel(blocks, caps, here_ref, row_ref, col_ref, table_ref, level_ref):
    lane = lax.broadcasted_iota(jnp.int32, (RB, blocks), 1)
    row = row_ref[...]
    alike = lax.broadcasted_iota(jnp.int32, (RB, blocks), 0) == row
    square = (blocks, blocks)
    upto = lax.broadcasted_iota(jnp.int32, square, 0) <= lax.broadcasted_iota(jnp.int32, square, 1)
    count = jnp.dot(alike.astype(jnp.float32), upto.astype(jnp.float32), preferred_element_type=jnp.float32)
    count = count.astype(jnp.int32)
    slot = jnp.sum(jnp.where(alike, count - 1, 0), axis=0, keepdims=True)
    source = lane[0:1] + col_ref[...]
    source = jnp.where(source >= blocks, source - blocks, source)
    needed = jnp.max(count)
    level = jnp.int32(0)
    tall, edges = jnp.int32(tiles_of(caps[0]) * 8), jnp.int32(16 * caps[0])
    for cap, following in zip(caps, caps[1:]):
        over = needed > cap
        level = level + over.astype(jnp.int32)
        tall = jnp.where(over, tiles_of(following) * 8, tall)
        edges = jnp.where(over, 16 * following, edges)
    level_ref[0] = level

    here = here_ref[0]
    edge_row = edges + (slot >> 3) * 8
    out_chunk = ((here + RB - row) & (RB - 1)) * tall
    in_chunk = ((here + row) & (RB - 1)) * tall
    turn = (lane[0:1] & 15) * EDGE + LANES - (slot & 7) * EDGE
    rows = (
        source * LANES,
        out_chunk + slot * 16,
        out_chunk + edge_row,
        slot & 7,
        in_chunk + slot * 16,
        in_chunk + edge_row,
        turn & (LANES - 1),
        (turn + LANES // 2) & (LANES - 1),
    )
    for k, values in enumerate(rows):
        table_ref[k : k + 1, :] = values


def index_of(row_offset, col_offset, here, caps):
    blocks = row_offset.shape[0]
    table, level = pl.pallas_call(
        functools.partial(index_kernel, blocks, caps),
        out_shape=(jax.ShapeDtypeStruct((8, blocks), jnp.int32), jax.ShapeDtypeStruct((1,), jnp.int32)),
        in_specs=[SMEM, VMEM, VMEM],
        out_specs=(VMEM, SMEM),
        name="block_index",
    )(here, row_offset.reshape(1, blocks), col_offset.reshape(1, blocks))
    return table, level[0]


def pack_kernel(blocks, cap, at_ref, p_in, out_hbm, p_ref, out_ref, in_sem, out_sem):
    width = blocks * LANES
    wide = width // 4
    loads = []
    for i in range(4):
        loads.append((pl.ds(i * wide, wide), pl.ds(LANES + i * wide, wide)))
    loads.append((pl.ds(width - LANES, LANES), pl.ds(0, LANES)))
    loads.append((pl.ds(0, LANES), pl.ds(width + LANES, LANES)))
    loads = [
        pltpu.make_async_copy(p_in.at[1, :, source], p_ref.at[:, target], in_sem.at[i])
        for i, (source, target) in enumerate(loads)
    ]
    for copy in loads:
        copy.start()
    lane = lanes_of(8)
    far = lane >= LANES // 2
    spots = lane // EDGE
    tall = tiles_of(cap) * 8
    for copy in loads:
        copy.wait()

    def block(b, _):
        col, row, edge_row, place = at_ref[0, b], at_ref[1, b], at_ref[2, b], at_ref[3, b]

        def of(i):
            return p_ref[:, pl.ds(pl.multiple_of(col + i * LANES, LANES), LANES)]

        out_ref[pl.ds(pl.multiple_of(row, 8), 16), :] = of(1)
        left, right = of(0), of(2)
        edge_rows = pl.ds(pl.multiple_of(edge_row, 8), 8)
        turn = place * EDGE + EDGE // 2
        for half in range(2):
            top = 8 * half
            edge = jnp.where(far, left[top : top + 8], right[top : top + 8])
            moved = pltpu.roll(edge, turn + half * (LANES // 2), 1)
            pltpu.store(out_ref.at[edge_rows, :], moved, mask=spots == place + 8 * half)
        return 0

    lax.fori_loop(0, blocks, block, 0, unroll=16)
    stores = []
    for i in range(RB):
        rows = pl.ds(i * tall, tall)
        stores.append(pltpu.make_async_copy(out_ref.at[rows, :], out_hbm.at[rows, :], out_sem.at[i]))
    for copy in stores:
        copy.start()
    for copy in stores:
        copy.wait()


def pack(cap, table, potentials):
    height, width = potentials.shape[1:]
    blocks = width // LANES
    shape = (RB * tiles_of(cap) * 8, LANES)
    return pl.pallas_call(
        functools.partial(pack_kernel, blocks, cap),
        out_shape=jax.ShapeDtypeStruct(shape, jnp.float32),
        in_specs=[SMEM, pl.BlockSpec(memory_space=pl.ANY)],
        out_specs=pl.BlockSpec(memory_space=pl.ANY),
        scratch_shapes=[
            pltpu.VMEM((height, width + 2 * LANES), jnp.float32),
            pltpu.VMEM(shape, jnp.float32),
            pltpu.SemaphoreType.DMA((6,)),
            pltpu.SemaphoreType.DMA((RB,)),
        ],
        compiler_params=params(24),
        cost_estimate=pl.CostEstimate(flops=2_000_000, bytes_accessed=3_000_000, transcendentals=0),
        name="pack_blocks",
    )(table, potentials)


def unpack_kernel(blocks, at_ref, in_ref, w_ref, h_ref, head_ref, tail_ref):
    spots = lanes_of(8) // EDGE

    def columns(group, _):
        edge_at = pl.multiple_of(group * 16, 16)
        for i in range(16):
            b = group * 16 + i
            row, edge_row, turn, half = at_ref[4, b], at_ref[5, b], at_ref[6, b], at_ref[7, b]
            tile = in_ref[pl.ds(pl.multiple_of(row, 8), 16), :]
            col = pl.ds(pl.multiple_of(b * LANES, LANES), LANES)
            w_ref[pl.ds(pl.multiple_of(b * 16, 16), 16), :] = tile
            head_ref[:, col] = tile[0:4]
            tail_ref[:, col] = tile[12:16]
            edge = in_ref[pl.ds(pl.multiple_of(edge_row, 8), 8), :]
            mask = spots == i
            pltpu.store(h_ref.at[pl.ds(edge_at, 8), :], pltpu.roll(edge, turn, 1), mask=mask)
            pltpu.store(h_ref.at[pl.ds(edge_at + 8, 8), :], pltpu.roll(edge, half, 1), mask=mask)
        return 0

    lax.fori_loop(0, blocks // 16, columns, 0)
    for g in range(blocks // 16):
        col = slice((blocks + g) * LANES, (blocks + g + 1) * LANES)
        head_ref[:, col] = h_ref[16 * g : 16 * g + 4, :]
        tail_ref[:, col] = h_ref[16 * g + 12 : 16 * g + 16, :]


def unpack(blocks, table, arrived):
    ends = jax.ShapeDtypeStruct((4, (blocks + blocks // 16) * LANES), jnp.float32)
    return pl.pallas_call(
        functools.partial(unpack_kernel, blocks),
        out_shape=(
            jax.ShapeDtypeStruct((blocks * 16, LANES), jnp.float32),
            jax.ShapeDtypeStruct((blocks, LANES), jnp.float32),
            ends,
            ends,
        ),
        in_specs=[SMEM, VMEM],
        out_specs=(VMEM,) * 4,
        compiler_params=params(24),
        cost_estimate=pl.CostEstimate(flops=2_000_000, bytes_accessed=3_000_000, transcendentals=0),
        name="unpack_blocks",
    )(table, arrived)


def edge_turn(b):
    return LANES - EDGE // 2 - b * EDGE


def columns_kernel(blocks, h_ref, w_ref, n0, n1, n2, n3, n4, c_ref, cc_ref, m0, m1, m2, m3, m4, g_ref, sem):
    lane = lanes_of(16)
    near = [pltpu.make_async_copy(n, m, sem.at[i]) for i, (n, m) in enumerate(zip((n0, n1, n2, n3, n4), (m0, m1, m2, m3, m4)))]
    for copy in near:
        copy.start()

    def spread(i, _):
        edge = h_ref[pl.ds(pl.multiple_of(i * 16, 16), 16), :]
        for k in range(16):
            g_ref[pl.ds(pl.multiple_of(i * 256 + k * 16, 16), 16), :] = pltpu.roll(edge, edge_turn(k), 1)
        return 0

    lax.fori_loop(0, blocks // 16, spread, 0, unroll=4)

    def block(b, _):
        tile = pl.ds(pl.multiple_of(b * 16, 16), 16)
        c_ref[tile, :], cc_ref[tile, :] = columns_of(w_ref[tile, :], g_ref[tile, :], lane)
        return 0

    lax.fori_loop(0, blocks, block, 0, unroll=16)
    for copy in near:
        copy.wait()


def far_columns(windows, edges, near):
    blocks = edges.shape[0]
    anywhere = pl.BlockSpec(memory_space=pl.ANY)
    out = pl.pallas_call(
        functools.partial(columns_kernel, blocks),
        out_shape=(jax.ShapeDtypeStruct(windows.shape, jnp.float32),) * 7,
        in_specs=[VMEM] * 2 + [anywhere] * 5,
        out_specs=(VMEM,) * 7,
        scratch_shapes=[
            pltpu.VMEM(windows.shape, jnp.float32),
            pltpu.SemaphoreType.DMA((5,)),
        ],
        compiler_params=params(16),
        cost_estimate=pl.CostEstimate(flops=20_000_000, bytes_accessed=3_000_000, transcendentals=0),
        name="far_columns",
    )(edges, windows, *near)
    return out[:2], out[2:]


def far_kernel(
    ratio_ref, w_ref, h_ref, up_ref, down_ref, far_c_ref, far_cc_ref, r_ref, c_ref, rr_ref, rc_ref, cc_ref,
    conv_out, shear_out, rot_out, disp_out, conv_ref, shear_ref, rot_ref, disp_ref, f_ref, e_ref, s_ref, sem,
):
    blocks = h_ref.shape[0]
    lane = lanes_of(16)
    near_to_two, near_to_source, two_to_source = ratio_ref[0], ratio_ref[1], ratio_ref[2]
    half_one, half_two = 0.5 * near_to_source, 0.5 * two_to_source
    refs = ((conv_ref, conv_out), (shear_ref, shear_out), (rot_ref, rot_out), (disp_ref, disp_out))

    def copies(group):
        cols = pl.ds(pl.multiple_of(group * 16 * LANES, 16 * LANES), 16 * LANES)
        return [
            pltpu.make_async_copy(ref.at[..., cols], out.at[..., cols], sem.at[k, group]) for k, (ref, out) in enumerate(refs)
        ]

    def columns(group, _):
        ends = pl.ds(pl.multiple_of((blocks + group) * LANES, LANES), LANES)
        e_ref[4:8, :] = up_ref[:, ends]
        e_ref[8:24, :] = h_ref[pl.ds(pl.multiple_of(group * 16, 16), 16), :]
        e_ref[24:28, :] = down_ref[:, ends]
        s_ref[...] = slope_rows(e_ref)

        def block(i, _):
            b = group * 16 + i
            col = pl.ds(pl.multiple_of(b * LANES, LANES), LANES)
            tile = pl.ds(pl.multiple_of(b * 16, 16), 16)
            window = f_ref.at[pl.ds(pl.multiple_of(i * STRIDE, STRIDE), STRIDE), :]
            window[4:8, :] = up_ref[:, col]
            window[8:24, :] = w_ref[tile, :]
            window[24:28, :] = down_ref[:, col]
            far_r, far_rr = rows_of(window)
            far_rc = column_slope(far_r, pltpu.roll(s_ref[...], edge_turn(i), 1), lane)
            far_cc = far_cc_ref[tile, :]
            near_rr, near_rc, near_cc = rr_ref[tile, :], rc_ref[tile, :], cc_ref[tile, :]
            inner_rr = 1.0 - near_to_two * near_rr
            inner_rc = -near_to_two * near_rc
            inner_cc = 1.0 - near_to_two * near_cc
            chain_rr = far_rr * inner_rr + far_rc * inner_rc
            chain_rc = far_rr * inner_rc + far_rc * inner_cc
            chain_cr = far_rc * inner_rr + far_cc * inner_rc
            chain_cc = far_rc * inner_rc + far_cc * inner_cc
            conv_ref[:, col] = half_one * (near_rr + near_cc) + half_two * (chain_rr + chain_cc)
            shear_ref[0, :, col] = half_one * (near_cc - near_rr) + half_two * (chain_cc - chain_rr)
            shear_ref[1, :, col] = near_to_source * near_rc + half_two * (chain_rc + chain_cr)
            rot_ref[:, col] = half_two * (chain_cr - chain_rc)
            disp_ref[0, :, col] = near_to_source * r_ref[tile, :] + two_to_source * far_r
            disp_ref[1, :, col] = near_to_source * c_ref[tile, :] + two_to_source * far_c_ref[tile, :]
            return 0

        lax.fori_loop(0, 16, block, 0, unroll=16)
        for copy in copies(group):
            copy.start()
        return 0

    lax.fori_loop(0, blocks // 16, columns, 0)

    def finish(group, _):
        for copy in copies(group):
            copy.wait()
        return 0

    lax.fori_loop(0, blocks // 16, finish, 0)


def assemble(ratios, windows, edges, above, below, far, near):
    blocks = edges.shape[0]
    flat = jax.ShapeDtypeStruct((16, blocks * LANES), jnp.float32)
    pair = jax.ShapeDtypeStruct((2, 16, blocks * LANES), jnp.float32)
    outs = (flat, pair, flat, pair)
    return pl.pallas_call(
        far_kernel,
        out_shape=outs,
        in_specs=[SMEM] + [VMEM] * 11,
        out_specs=(pl.BlockSpec(memory_space=pl.ANY),) * 4,
        scratch_shapes=[pltpu.VMEM(o.shape, o.dtype) for o in outs]
        + [
            pltpu.VMEM((16 * STRIDE, LANES), jnp.float32),
            pltpu.VMEM((STRIDE, LANES), jnp.float32),
            pltpu.VMEM((16, LANES), jnp.float32),
            pltpu.SemaphoreType.DMA((4, blocks // 16)),
        ],
        compiler_params=params(16),
        cost_estimate=pl.CostEstimate(flops=40_000_000, bytes_accessed=6_000_000, transcendentals=0),
        name="far_fields",
    )(ratios, windows, edges, above, below, *far, *near)


def passed(x, by):
    size = lax.axis_size("row")
    return lax.ppermute(x, "row", [(i, (i + by) % size) for i in range(size)])


def near_plane(potentials):
    height = potentials.shape[1]
    above = passed(potentials[0, height - 4 :, :], 1)
    below = passed(potentials[0, :4, :], -1)
    return near_fields(potentials, above, below)


def near_blank(potentials):
    width = potentials.shape[2]
    return (jnp.zeros((width // LANES * 16, LANES), jnp.float32),) * 5


def exchange(cap, groups, potentials, here, table):
    blocks = potentials.shape[2] // LANES
    packed = pack(cap, table, potentials)
    packed = packed.reshape(RB, tiles_of(cap) * 8, LANES)
    arrived = lax.all_to_all(packed, "row", 0, 0, axis_index_groups=groups)
    near = lax.cond(here[0] >= 0, near_plane, near_blank, potentials)
    arrived = arrived.reshape(RB * tiles_of(cap) * 8, LANES)
    return unpack(blocks, table, arrived), near


def per_device(potentials, ratios, row_offset, col_offset):
    stride = lax.axis_size("row") // RB
    blocks = potentials.shape[2] // LANES
    caps = tuple(c for c in CAPS if c < blocks) + (blocks,)
    here = (lax.axis_index("row") // stride).astype(jnp.int32).reshape(1)
    table, level = index_of(row_offset, col_offset, here, caps)
    groups = [[y * stride + j for y in range(RB)] for j in range(stride)]
    (windows, edges, heads, tails), near = lax.switch(
        level,
        [functools.partial(exchange, cap, groups) for cap in caps],
        potentials, here, table,
    )
    above = passed(tails, 1)
    below = passed(heads, -1)
    far, near = far_columns(windows, edges, near)
    return assemble(ratios, windows, edges, above, below, far, near)


def solution(mesh):
    return jax.shard_map(
        per_device,
        mesh=mesh,
        in_specs=(P("cosmo", "row", None), P("cosmo"), P("cosmo"), P("cosmo")),
        out_specs=(
            P(("cosmo", "row"), None),
            P(None, ("cosmo", "row"), None),
            P(("cosmo", "row"), None),
            P(None, ("cosmo", "row"), None),
        ),
        check_vma=False,
    )
```

```python
import functools

import jax
import jax.numpy as jnp
from jax import lax
from jax.experimental import pallas as pl
from jax.experimental.pallas import tpu as pltpu
from jax.sharding import PartitionSpec as P

RB = 8
LANES = 128
EDGE = 8
STRIDE = 32
CAPS = (21, 22, 23, 24, 25, 26, 28, 32)
C1, C2 = 8.0 / 12.0, 1.0 / 12.0
VMEM = pl.BlockSpec(memory_space=pltpu.VMEM)
SMEM = pl.BlockSpec(memory_space=pltpu.SMEM)


def lanes_of(rows):
    return lax.broadcasted_iota(jnp.int32, (rows, LANES), 1)


def params(mib):
    return pltpu.CompilerParams(vmem_limit_bytes=mib * 2**20)


def tiles_of(cap):
    return 2 * cap + -(-cap // 8)


def first(ahead, behind, ahead2, behind2):
    return C1 * (ahead - behind) - C2 * (ahead2 - behind2)


def second(centre, pairs):
    one, two, three, four = pairs
    return (four - 16.0 * three + 64.0 * two + 16.0 * one - 130.0 * centre) * (1.0 / 144.0)


def rows_of(window):
    def at(k):
        return window[8 + k : 24 + k, :]

    a1, b1, a2, b2 = at(1), at(-1), at(2), at(-2)
    slope = first(a1, b1, a2, b2)
    curve = second(at(0), (a1 + b1, a2 + b2, at(3) + at(-3), at(4) + at(-4)))
    return slope, curve


def slope_rows(window):
    def at(k):
        return window[8 + k : 24 + k, :]

    return first(at(1), at(-1), at(2), at(-2))


def shifted(field, beside, k, lane):
    if k > 0:
        return pltpu.roll(jnp.where(lane < k, beside, field), LANES - k, 1)
    return pltpu.roll(jnp.where(lane >= LANES + k, beside, field), -k, 1)


def columns_of(field, beside, lane):
    def at(k):
        return shifted(field, beside, k, lane)

    a1, b1, a2, b2 = at(1), at(-1), at(2), at(-2)
    slope_c = first(a1, b1, a2, b2)
    curve_cc = second(field, (a1 + b1, a2 + b2, at(3) + at(-3), at(4) + at(-4)))
    return slope_c, curve_cc


def column_slope(field, beside, lane):
    def at(k):
        return shifted(field, beside, k, lane)

    return first(at(1), at(-1), at(2), at(-2))


def near_kernel(blocks, p_ref, up_ref, down_ref, r_ref, c_ref, rr_ref, rc_ref, cc_ref, f_ref):
    lane = lanes_of(16)

    def rows(b, _):
        col = pl.multiple_of(b * LANES, LANES)
        base = pl.multiple_of(b * STRIDE, STRIDE)
        out = pl.multiple_of(b * 16, 16)
        window = f_ref.at[pl.ds(base, STRIDE), :]
        window[4:8, :] = up_ref[:, pl.ds(col, LANES)]
        window[8:24, :] = p_ref[:, pl.ds(col, LANES)]
        window[24:28, :] = down_ref[:, pl.ds(col, LANES)]
        slope, curve = rows_of(window)
        r_ref[pl.ds(out, 16), :] = slope
        rr_ref[pl.ds(out, 16), :] = curve
        return 0

    lax.fori_loop(0, blocks, rows, 0, unroll=8)

    def columns(b, _):
        before = lax.rem(b + (blocks - 1), blocks)
        after = lax.rem(b + 1, blocks)

        def of(i):
            return p_ref[:, pl.ds(pl.multiple_of(i * LANES, LANES), LANES)]

        def slope_of(i):
            return r_ref[pl.ds(pl.multiple_of(i * 16, 16), 16), :]

        far = lane >= LANES // 2
        slope_c, curve_cc = columns_of(of(b), jnp.where(far, of(before), of(after)), lane)
        curve_rc = column_slope(slope_of(b), jnp.where(far, slope_of(before), slope_of(after)), lane)
        out = pl.ds(pl.multiple_of(b * 16, 16), 16)
        c_ref[out, :] = slope_c
        rc_ref[out, :] = curve_rc
        cc_ref[out, :] = curve_cc
        return 0

    lax.fori_loop(0, blocks, columns, 0, unroll=8)


def near_fields(potentials, up, down):
    height, width = potentials.shape[1:]
    blocks = width // LANES
    shape = jax.ShapeDtypeStruct((blocks * 16, LANES), jnp.float32)
    return pl.pallas_call(
        functools.partial(near_kernel, blocks),
        grid=(1,),
        out_shape=(shape,) * 5,
        in_specs=[pl.BlockSpec((None, height, width), lambda i: (0, 0, 0)), VMEM, VMEM],
        out_specs=(VMEM,) * 5,
        scratch_shapes=[pltpu.VMEM((blocks * STRIDE, LANES), jnp.float32)],
        compiler_params=params(16),
        cost_estimate=pl.CostEstimate(flops=60_000_000, bytes_accessed=7_000_000, transcendentals=0),
        name="near_fields",
    )(potentials, up, down)


def index_kernel(blocks, caps, here_ref, row_ref, col_ref, table_ref, level_ref):
    lane = lax.broadcasted_iota(jnp.int32, (RB, blocks), 1)
    row = row_ref[...]
    alike = lax.broadcasted_iota(jnp.int32, (RB, blocks), 0) == row
    square = (blocks, blocks)
    upto = lax.broadcasted_iota(jnp.int32, square, 0) <= lax.broadcasted_iota(jnp.int32, square, 1)
    count = jnp.dot(alike.astype(jnp.float32), upto.astype(jnp.float32), preferred_element_type=jnp.float32)
    count = count.astype(jnp.int32)
    slot = jnp.sum(jnp.where(alike, count - 1, 0), axis=0, keepdims=True)
    source = lane[0:1] + col_ref[...]
    source = jnp.where(source >= blocks, source - blocks, source)
    needed = jnp.max(count)
    level = jnp.int32(0)
    tall, edges = jnp.int32(tiles_of(caps[0]) * 8), jnp.int32(16 * caps[0])
    for cap, following in zip(caps, caps[1:]):
        over = needed > cap
        level = level + over.astype(jnp.int32)
        tall = jnp.where(over, tiles_of(following) * 8, tall)
        edges = jnp.where(over, 16 * following, edges)
    level_ref[0] = level

    here = here_ref[0]
    edge_row = edges + (slot >> 3) * 8
    out_chunk = ((here + RB - row) & (RB - 1)) * tall
    in_chunk = ((here + row) & (RB - 1)) * tall
    turn = (lane[0:1] & 15) * EDGE + LANES - (slot & 7) * EDGE
    rows = (
        source * LANES,
        out_chunk + slot * 16,
        out_chunk + edge_row,
        slot & 7,
        in_chunk + slot * 16,
        in_chunk + edge_row,
        turn & (LANES - 1),
        (turn + LANES // 2) & (LANES - 1),
    )
    for k, values in enumerate(rows):
        table_ref[k : k + 1, :] = values


def index_of(row_offset, col_offset, here, caps):
    blocks = row_offset.shape[0]
    table, level = pl.pallas_call(
        functools.partial(index_kernel, blocks, caps),
        out_shape=(jax.ShapeDtypeStruct((8, blocks), jnp.int32), jax.ShapeDtypeStruct((1,), jnp.int32)),
        in_specs=[SMEM, VMEM, VMEM],
        out_specs=(VMEM, SMEM),
        name="block_index",
    )(here, row_offset.reshape(1, blocks), col_offset.reshape(1, blocks))
    return table, level[0]


def pack_kernel(blocks, cap, at_ref, p_in, out_hbm, p_ref, out_ref, in_sem, out_sem):
    width = blocks * LANES
    wide = width // 4
    loads = []
    for i in range(4):
        loads.append((pl.ds(i * wide, wide), pl.ds(LANES + i * wide, wide)))
    loads.append((pl.ds(width - LANES, LANES), pl.ds(0, LANES)))
    loads.append((pl.ds(0, LANES), pl.ds(width + LANES, LANES)))
    loads = [
        pltpu.make_async_copy(p_in.at[1, :, source], p_ref.at[:, target], in_sem.at[i])
        for i, (source, target) in enumerate(loads)
    ]
    for copy in loads:
        copy.start()
    lane = lanes_of(8)
    far = lane >= LANES // 2
    spots = lane // EDGE
    tall = tiles_of(cap) * 8
    for copy in loads:
        copy.wait()

    def block(b, _):
        col, row, edge_row, place = at_ref[0, b], at_ref[1, b], at_ref[2, b], at_ref[3, b]

        def of(i):
            return p_ref[:, pl.ds(pl.multiple_of(col + i * LANES, LANES), LANES)]

        out_ref[pl.ds(pl.multiple_of(row, 8), 16), :] = of(1)
        left, right = of(0), of(2)
        edge_rows = pl.ds(pl.multiple_of(edge_row, 8), 8)
        turn = place * EDGE + EDGE // 2
        for half in range(2):
            top = 8 * half
            edge = jnp.where(far, left[top : top + 8], right[top : top + 8])
            moved = pltpu.roll(edge, turn + half * (LANES // 2), 1)
            pltpu.store(out_ref.at[edge_rows, :], moved, mask=spots == place + 8 * half)
        return 0

    lax.fori_loop(0, blocks, block, 0, unroll=16)
    stores = []
    for i in range(RB):
        rows = pl.ds(i * tall, tall)
        stores.append(pltpu.make_async_copy(out_ref.at[rows, :], out_hbm.at[rows, :], out_sem.at[i]))
    for copy in stores:
        copy.start()
    for copy in stores:
        copy.wait()


def pack(cap, table, potentials):
    height, width = potentials.shape[1:]
    blocks = width // LANES
    shape = (RB * tiles_of(cap) * 8, LANES)
    return pl.pallas_call(
        functools.partial(pack_kernel, blocks, cap),
        out_shape=jax.ShapeDtypeStruct(shape, jnp.float32),
        in_specs=[SMEM, pl.BlockSpec(memory_space=pl.ANY)],
        out_specs=pl.BlockSpec(memory_space=pl.ANY),
        scratch_shapes=[
            pltpu.VMEM((height, width + 2 * LANES), jnp.float32),
            pltpu.VMEM(shape, jnp.float32),
            pltpu.SemaphoreType.DMA((6,)),
            pltpu.SemaphoreType.DMA((RB,)),
        ],
        compiler_params=params(24),
        cost_estimate=pl.CostEstimate(flops=2_000_000, bytes_accessed=3_000_000, transcendentals=0),
        name="pack_blocks",
    )(table, potentials)


def unpack_kernel(blocks, at_ref, in_ref, w_ref, h_ref):
    spots = lanes_of(8) // EDGE

    def columns(group, _):
        edge_at = pl.multiple_of(group * 16, 16)
        for i in range(16):
            b = group * 16 + i
            row, edge_row, turn, half = at_ref[4, b], at_ref[5, b], at_ref[6, b], at_ref[7, b]
            tile = in_ref[pl.ds(pl.multiple_of(row, 8), 16), :]
            w_ref[pl.ds(pl.multiple_of(b * 16, 16), 16), :] = tile
            edge = in_ref[pl.ds(pl.multiple_of(edge_row, 8), 8), :]
            mask = spots == i
            pltpu.store(h_ref.at[pl.ds(edge_at, 8), :], pltpu.roll(edge, turn, 1), mask=mask)
            pltpu.store(h_ref.at[pl.ds(edge_at + 8, 8), :], pltpu.roll(edge, half, 1), mask=mask)
        return 0

    lax.fori_loop(0, blocks // 16, columns, 0)


def unpack(blocks, table, arrived):
    return pl.pallas_call(
        functools.partial(unpack_kernel, blocks),
        out_shape=(
            jax.ShapeDtypeStruct((blocks * 16, LANES), jnp.float32),
            jax.ShapeDtypeStruct((blocks, LANES), jnp.float32),
        ),
        in_specs=[SMEM, VMEM],
        out_specs=(VMEM,) * 2,
        compiler_params=params(24),
        cost_estimate=pl.CostEstimate(flops=2_000_000, bytes_accessed=3_000_000, transcendentals=0),
        name="unpack_blocks",
    )(table, arrived)


def ends_kernel(blocks, w_ref, h_ref, head_ref, tail_ref):
    def block(b, _):
        tile = w_ref[pl.ds(pl.multiple_of(b * 16, 16), 16), :]
        col = pl.ds(pl.multiple_of(b * LANES, LANES), LANES)
        head_ref[:, col] = tile[0:4]
        tail_ref[:, col] = tile[12:16]
        return 0

    lax.fori_loop(0, blocks, block, 0, unroll=16)
    for g in range(blocks // 16):
        col = slice((blocks + g) * LANES, (blocks + g + 1) * LANES)
        head_ref[:, col] = h_ref[16 * g : 16 * g + 4, :]
        tail_ref[:, col] = h_ref[16 * g + 12 : 16 * g + 16, :]


def ends_of(windows, edges):
    blocks = edges.shape[0]
    ends = jax.ShapeDtypeStruct((4, (blocks + blocks // 16) * LANES), jnp.float32)
    return pl.pallas_call(
        functools.partial(ends_kernel, blocks),
        out_shape=(ends, ends),
        in_specs=[VMEM, VMEM],
        out_specs=(VMEM, VMEM),
        compiler_params=params(8),
        cost_estimate=pl.CostEstimate(flops=100_000, bytes_accessed=1_600_000, transcendentals=0),
        name="row_ends",
    )(windows, edges)


def edge_turn(b):
    return LANES - EDGE // 2 - b * EDGE


def columns_kernel(blocks, h_ref, w_ref, n0, n1, n2, n3, n4, c_ref, cc_ref, m0, m1, m2, m3, m4, g_ref, sem):
    lane = lanes_of(16)
    near = [pltpu.make_async_copy(n, m, sem.at[i]) for i, (n, m) in enumerate(zip((n0, n1, n2, n3, n4), (m0, m1, m2, m3, m4)))]
    for copy in near:
        copy.start()

    def spread(i, _):
        edge = h_ref[pl.ds(pl.multiple_of(i * 16, 16), 16), :]
        for k in range(16):
            g_ref[pl.ds(pl.multiple_of(i * 256 + k * 16, 16), 16), :] = pltpu.roll(edge, edge_turn(k), 1)
        return 0

    lax.fori_loop(0, blocks // 16, spread, 0, unroll=4)

    def block(b, _):
        tile = pl.ds(pl.multiple_of(b * 16, 16), 16)
        c_ref[tile, :], cc_ref[tile, :] = columns_of(w_ref[tile, :], g_ref[tile, :], lane)
        return 0

    lax.fori_loop(0, blocks, block, 0, unroll=16)
    for copy in near:
        copy.wait()


def far_columns(windows, edges, near):
    blocks = edges.shape[0]
    anywhere = pl.BlockSpec(memory_space=pl.ANY)
    out = pl.pallas_call(
        functools.partial(columns_kernel, blocks),
        out_shape=(jax.ShapeDtypeStruct(windows.shape, jnp.float32),) * 7,
        in_specs=[VMEM] * 2 + [anywhere] * 5,
        out_specs=(VMEM,) * 7,
        scratch_shapes=[
            pltpu.VMEM(windows.shape, jnp.float32),
            pltpu.SemaphoreType.DMA((5,)),
        ],
        compiler_params=params(16),
        cost_estimate=pl.CostEstimate(flops=20_000_000, bytes_accessed=3_000_000, transcendentals=0),
        name="far_columns",
    )(edges, windows, *near)
    return out[:2], out[2:]


def far_kernel(
    ratio_ref, w_ref, h_ref, up_ref, down_ref, far_c_ref, far_cc_ref, r_ref, c_ref, rr_ref, rc_ref, cc_ref,
    conv_out, shear_out, rot_out, disp_out, conv_ref, shear_ref, rot_ref, disp_ref, f_ref, e_ref, s_ref, sem,
):
    blocks = h_ref.shape[0]
    lane = lanes_of(16)
    near_to_two, near_to_source, two_to_source = ratio_ref[0], ratio_ref[1], ratio_ref[2]
    half_one, half_two = 0.5 * near_to_source, 0.5 * two_to_source
    refs = ((conv_ref, conv_out), (shear_ref, shear_out), (rot_ref, rot_out), (disp_ref, disp_out))

    def copies(group):
        cols = pl.ds(pl.multiple_of(group * 16 * LANES, 16 * LANES), 16 * LANES)
        return [
            pltpu.make_async_copy(ref.at[..., cols], out.at[..., cols], sem.at[k, group]) for k, (ref, out) in enumerate(refs)
        ]

    def columns(group, _):
        ends = pl.ds(pl.multiple_of((blocks + group) * LANES, LANES), LANES)
        e_ref[4:8, :] = up_ref[:, ends]
        e_ref[8:24, :] = h_ref[pl.ds(pl.multiple_of(group * 16, 16), 16), :]
        e_ref[24:28, :] = down_ref[:, ends]
        s_ref[...] = slope_rows(e_ref)

        def block(i, _):
            b = group * 16 + i
            col = pl.ds(pl.multiple_of(b * LANES, LANES), LANES)
            tile = pl.ds(pl.multiple_of(b * 16, 16), 16)
            window = f_ref.at[pl.ds(pl.multiple_of(i * STRIDE, STRIDE), STRIDE), :]
            window[4:8, :] = up_ref[:, col]
            window[8:24, :] = w_ref[tile, :]
            window[24:28, :] = down_ref[:, col]
            far_r, far_rr = rows_of(window)
            far_rc = column_slope(far_r, pltpu.roll(s_ref[...], edge_turn(i), 1), lane)
            far_cc = far_cc_ref[tile, :]
            near_rr, near_rc, near_cc = rr_ref[tile, :], rc_ref[tile, :], cc_ref[tile, :]
            inner_rr = 1.0 - near_to_two * near_rr
            inner_rc = -near_to_two * near_rc
            inner_cc = 1.0 - near_to_two * near_cc
            chain_rr = far_rr * inner_rr + far_rc * inner_rc
            chain_rc = far_rr * inner_rc + far_rc * inner_cc
            chain_cr = far_rc * inner_rr + far_cc * inner_rc
            chain_cc = far_rc * inner_rc + far_cc * inner_cc
            conv_ref[:, col] = half_one * (near_rr + near_cc) + half_two * (chain_rr + chain_cc)
            shear_ref[0, :, col] = half_one * (near_cc - near_rr) + half_two * (chain_cc - chain_rr)
            shear_ref[1, :, col] = near_to_source * near_rc + half_two * (chain_rc + chain_cr)
            rot_ref[:, col] = half_two * (chain_cr - chain_rc)
            disp_ref[0, :, col] = near_to_source * r_ref[tile, :] + two_to_source * far_r
            disp_ref[1, :, col] = near_to_source * c_ref[tile, :] + two_to_source * far_c_ref[tile, :]
            return 0

        lax.fori_loop(0, 16, block, 0, unroll=16)
        for copy in copies(group):
            copy.start()
        return 0

    lax.fori_loop(0, blocks // 16, columns, 0)

    def finish(group, _):
        for copy in copies(group):
            copy.wait()
        return 0

    lax.fori_loop(0, blocks // 16, finish, 0)


def assemble(ratios, windows, edges, above, below, far, near):
    blocks = edges.shape[0]
    flat = jax.ShapeDtypeStruct((16, blocks * LANES), jnp.float32)
    pair = jax.ShapeDtypeStruct((2, 16, blocks * LANES), jnp.float32)
    outs = (flat, pair, flat, pair)
    return pl.pallas_call(
        far_kernel,
        out_shape=outs,
        in_specs=[SMEM] + [VMEM] * 11,
        out_specs=(pl.BlockSpec(memory_space=pl.ANY),) * 4,
        scratch_shapes=[pltpu.VMEM(o.shape, o.dtype) for o in outs]
        + [
            pltpu.VMEM((16 * STRIDE, LANES), jnp.float32),
            pltpu.VMEM((STRIDE, LANES), jnp.float32),
            pltpu.VMEM((16, LANES), jnp.float32),
            pltpu.SemaphoreType.DMA((4, blocks // 16)),
        ],
        compiler_params=params(16),
        cost_estimate=pl.CostEstimate(flops=40_000_000, bytes_accessed=6_000_000, transcendentals=0),
        name="far_fields",
    )(ratios, windows, edges, above, below, *far, *near)


def passed(x, by):
    size = lax.axis_size("row")
    return lax.ppermute(x, "row", [(i, (i + by) % size) for i in range(size)])


def near_plane(potentials):
    height = potentials.shape[1]
    above = passed(potentials[0, height - 4 :, :], 1)
    below = passed(potentials[0, :4, :], -1)
    return near_fields(potentials, above, below)


def near_blank(potentials):
    width = potentials.shape[2]
    return (jnp.zeros((width // LANES * 16, LANES), jnp.float32),) * 5


def exchange(cap, groups, potentials, here, table):
    blocks = potentials.shape[2] // LANES
    packed = pack(cap, table, potentials)
    packed = packed.reshape(RB, tiles_of(cap) * 8, LANES)
    arrived = lax.all_to_all(packed, "row", 0, 0, axis_index_groups=groups)
    near = lax.cond(here[0] >= 0, near_plane, near_blank, potentials)
    arrived = arrived.reshape(RB * tiles_of(cap) * 8, LANES)
    return unpack(blocks, table, arrived), near


def per_device(potentials, ratios, row_offset, col_offset):
    stride = lax.axis_size("row") // RB
    blocks = potentials.shape[2] // LANES
    caps = tuple(c for c in CAPS if c < blocks) + (blocks,)
    here = (lax.axis_index("row") // stride).astype(jnp.int32).reshape(1)
    table, level = index_of(row_offset, col_offset, here, caps)
    groups = [[y * stride + j for y in range(RB)] for j in range(stride)]
    (windows, edges), near = lax.switch(
        level,
        [functools.partial(exchange, cap, groups) for cap in caps],
        potentials, here, table,
    )
    heads, tails = ends_of(windows, edges)
    above = passed(tails, 1)
    below = passed(heads, -1)
    far, near = far_columns(windows, edges, near)
    return assemble(ratios, windows, edges, above, below, far, near)


def solution(mesh):
    return jax.shard_map(
        per_device,
        mesh=mesh,
        in_specs=(P("cosmo", "row", None), P("cosmo"), P("cosmo"), P("cosmo")),
        out_specs=(
            P(("cosmo", "row"), None),
            P(None, ("cosmo", "row"), None),
            P(("cosmo", "row"), None),
            P(None, ("cosmo", "row"), None),
        ),
        check_vma=False,
    )
```
